32 devices in a mesh: groups: 2 (over x), hid: 16 (over z, y, core).
Axes of the slice: x: 2, y: 2, z: 4, core: 2. Of those that a mesh axis runs over, the one named last changes fastest.
Arguments:
- queries: bfloat16 [128, 64, 128], P(('groups', 'hid')), parts along dimension 0, may hold values from -12 to 12
- k_cache: bfloat16 [128, 192, 1024], P(('groups', 'hid')), parts along dimension 0, may hold values from -450 to 450
- v_cache: bfloat16 [128, 192, 1024], P(('groups', 'hid')), parts along dimension 0, may hold values from -6 to 6
- lengths: int32 [128], P(('groups', 'hid')), parts along dimension 0, may hold values from 24 to 192, as said below
- residual_in: bfloat16 [128, 8192], P(('groups', 'hid')), parts along dimension 0, may hold values from -6 to 6
- norm_gain: float32 [8192], replicated, may hold values from 0.25 to 1.75
- gate_w: bfloat16 [16, 56, 1024, 128], P('hid'), may hold values from -0.0625 to 0.0625
- up_w: bfloat16 [16, 56, 1024, 128], P('hid'), may hold values from -0.0625 to 0.0625
- down_w: bfloat16 [16, 56, 128, 1024], P('hid'), may hold values from -0.09375 to 0.09375
- block_list: int32 [4, 28], P('groups'), parts along dimension 0, may hold values from 0 to 55, as said below
- block_count: int32 [4], P('groups'), parts along dimension 0, may hold values from 1 to 28, as said below
Outputs:
- layer_out: bfloat16 [128, 8192], P(('groups', 'hid')), parts along dimension 0
The draws below stay inside these ranges and needn't reach their ends.
There are 2 independent parts, one for each index of `groups`. The reference program is written for one: setup_inputs(seed, part) draws one part's arguments, and reference() takes and returns one part's arrays. A program takes and returns all parts, laid end to end along the dimension named above; an argument that names none is the same for every part. Nothing has to cross between parts.
Inputs may be any that keep to these rules, and one draw needn't show every extreme that they name: `lengths`: some request's length is 192. `block_list`: each row holds 28 distinct block indices of its group. `block_count`: exactly one group has all 28 listed blocks active.
All inputs are finite; a program needn't handle non-finite values.
Results may differ from the reference program's by a relative error of at most 0.006.
Values may be sent and summed in bfloat16 or wider, within the bound.
A program may use at most 128 MiB of HBM per device.

```python
import math
import jax
import jax.numpy as jnp
from jax import lax

D = 8192
H = 64
KV = 8
HD = 128
BW = 128
MDL = 8
REQ_DEV = 4
CACHE = 192
HG = 2
DS = 1024
BLK_G = 56
CAP = 28
BATCH = 64
N_HID = 16


def query_key_pair(key):
    query_stream = jax.random.fold_in(key, 11)
    cache_stream = jax.random.fold_in(key, 12)
    query_vals = jnp.clip(jax.random.normal(query_stream, (BATCH, H, HD), jnp.float32), -6.0, 6.0)
    key_vals = jnp.clip(jax.random.normal(cache_stream, (BATCH, CACHE, KV, HD), jnp.float32), -6.0, 6.0)
    return (query_vals, key_vals.reshape(BATCH, CACHE, KV * HD))


def draw_queries(key, part):
    return query_key_pair(key)[0].astype(jnp.bfloat16)


def draw_k_cache(key, part):
    return query_key_pair(key)[1].astype(jnp.bfloat16)


def draw_lengths(key, part):
    length_stream = jax.random.fold_in(key, 21)
    drawn = jax.random.randint(length_stream, (BATCH,), max(2, CACHE // 8), CACHE + 1, jnp.int32)
    full_row = jax.random.randint(jax.random.fold_in(length_stream, 1), (), 0, BATCH, jnp.int32)
    return jnp.where(jnp.arange(BATCH, dtype=jnp.int32) == full_row, CACHE, drawn).astype(jnp.int32)


def draw_block_list(key, part):
    table_stream = jax.random.fold_in(key, 31)
    row_streams = jax.random.split(table_stream, HG)
    rows_all = jax.vmap(lambda stream: jax.random.permutation(stream, BLK_G)[:CAP])(row_streams).astype(jnp.int32)
    first_row = rows_all[0]
    held = first_row[0]
    first_row = jnp.where(first_row == BLK_G - 1, held, first_row)
    first_row = first_row.at[0].set(BLK_G - 1)
    second = first_row[1]
    first_row = jnp.where(first_row == 0, second, first_row)
    first_row = first_row.at[1].set(0)
    return rows_all.at[0].set(first_row)


def draw_block_count(key, part):
    count_stream = jax.random.fold_in(key, 47)
    counts = jax.random.randint(jax.random.fold_in(count_stream, 3), (HG,), 1, CAP, jnp.int32)
    full_group = jax.random.randint(jax.random.fold_in(count_stream, 5), (), 0, HG, jnp.int32)
    return jnp.where(jnp.arange(HG, dtype=jnp.int32) == full_group, CAP, counts).astype(jnp.int32)


def levels(own_key, extent, pieces, low, high):
    loudness = 1.0
    for axis_at, blocks in pieces:
        draws = jax.random.uniform(jax.random.fold_in(jax.random.fold_in(own_key, 6), axis_at), (blocks,), jnp.float32, low / len(pieces), high / len(pieces))
        loudness = loudness * jnp.repeat(jnp.exp(draws), extent[axis_at] // blocks).reshape((-1,) + (1,) * (len(extent) - 1 - axis_at))
    return loudness


def gaussian(own_key, extent, deviation, most, cuts=(), kind=jnp.bfloat16):
    loudness = levels(own_key, extent, cuts, -0.22, 0.18) if cuts else 1.0
    array = jax.random.normal(own_key, extent, jnp.float32) * deviation * loudness
    return jnp.minimum(jnp.maximum(array, -most), most).astype(kind)


def setup_inputs(seed: int = 0, part: int = 0) -> dict:
    streams_of = jax.random.split(jax.random.key(seed), 12)
    part_splits = jax.random.split(jax.random.fold_in(streams_of[11], part), 12)
    queries = draw_queries(jax.random.fold_in(jax.random.fold_in(streams_of[11], part), 71), part)
    k_cache = draw_k_cache(jax.random.fold_in(jax.random.fold_in(streams_of[11], part), 71), part)
    v_cache = gaussian(part_splits[2], (BATCH, CACHE, KV * HD), 1.0, 6.0, ((0, 16),))
    lengths = draw_lengths(jax.random.fold_in(jax.random.fold_in(streams_of[11], part), 71), part)
    residual_in = gaussian(part_splits[4], (BATCH, D), 1.0, 6.0, ((0, 16),))
    norm_gain = jnp.clip(1.0 + 0.15 * jax.random.normal(streams_of[5], (D,), jnp.float32), 0.25, 1.75)
    gate_w = gaussian(streams_of[6], (N_HID, BLK_G, DS, BW), D ** -0.5, 0.0625, ((0, 16),))
    up_w = gaussian(streams_of[7], (N_HID, BLK_G, DS, BW), D ** -0.5, 0.0625, ((0, 16),))
    down_w = gaussian(streams_of[8], (N_HID, BLK_G, BW, DS), (CAP * BW * HG // 2) ** -0.5, 0.09375, ((0, 16),))
    block_list = draw_block_list(jax.random.fold_in(jax.random.fold_in(streams_of[11], part), 71), part)
    block_count = draw_block_count(jax.random.fold_in(jax.random.fold_in(streams_of[11], part), 71), part)
    return dict(queries=queries, k_cache=k_cache, v_cache=v_cache, lengths=lengths, residual_in=residual_in, norm_gain=norm_gain, gate_w=gate_w, up_w=up_w, down_w=down_w, block_list=block_list, block_count=block_count)


def attend_block(parts):
    query_part, key_part, value_part, length_part = parts
    rows_here = query_part.shape[0]
    query_f = query_part.astype(jnp.float32).reshape(rows_here, KV, H // KV, HD)
    key_f = key_part.astype(jnp.float32).reshape(rows_here, CACHE, KV, HD)
    value_f = value_part.astype(jnp.float32).reshape(rows_here, CACHE, KV, HD)
    scores = jnp.einsum('rkgd,rtkd->rkgt', query_f, key_f) / math.sqrt(HD)
    valid = jnp.arange(CACHE)[None, None, None, :] < length_part[:, None, None, None]
    scores = jnp.where(valid, scores, -1e+30)
    row_top = lax.optimization_barrier(jnp.max(scores, axis=-1, keepdims=True))
    exp_terms = jnp.where(valid, jnp.exp(scores - row_top), 0.0)
    attn_probs = (exp_terms / lax.optimization_barrier(jnp.sum(exp_terms, axis=-1, keepdims=True))).astype(jnp.bfloat16)
    attended = jnp.einsum('rkgt,rtkd->rkgd', attn_probs.astype(jnp.float32), value_f)
    return attended.reshape(rows_here, D)

def select_blocks(tiles, block_list):
    return jax.vmap(lambda tile_set, chosen: jnp.take(tile_set, chosen, axis=1))(tiles, block_list)

def reference(queries, k_cache, v_cache, lengths, residual_in, norm_gain, gate_w, up_w, down_w, block_list, block_count):
    attended = lax.map(attend_block, (queries.reshape(N_HID, REQ_DEV, H, HD), k_cache.reshape(N_HID, REQ_DEV, CACHE, KV * HD), v_cache.reshape(N_HID, REQ_DEV, CACHE, KV * HD), lengths.reshape(N_HID, REQ_DEV))).reshape(BATCH, D)
    mixed_rows = residual_in.astype(jnp.float32) + attended
    mean_sq = lax.optimization_barrier(jnp.mean(mixed_rows * mixed_rows, axis=1, keepdims=True))
    normed = (mixed_rows * lax.rsqrt(mean_sq + 1e-05) * norm_gain).astype(jnp.bfloat16)
    normed_f = normed.astype(jnp.float32).reshape(BATCH, MDL, DS)
    gate_sel = select_blocks(gate_w.reshape(HG, MDL, BLK_G, DS, BW), block_list).astype(jnp.float32)
    up_sel = select_blocks(up_w.reshape(HG, MDL, BLK_G, DS, BW), block_list).astype(jnp.float32)
    down_sel = select_blocks(down_w.reshape(HG, MDL, BLK_G, BW, DS), block_list).astype(jnp.float32)
    gate_pre = jnp.einsum('bms,gmcsu->bgcu', normed_f, gate_sel)
    up_pre = jnp.einsum('bms,gmcsu->bgcu', normed_f, up_sel)
    active = jnp.arange(CAP)[None, :] < block_count[:, None]
    hidden = jnp.where(active[None, :, :, None], jnp.maximum(gate_pre, 0.0) * up_pre, 0.0).astype(jnp.bfloat16)
    ffn_out = jnp.einsum('bgcu,gmcus->bms', hidden.astype(jnp.float32), down_sel).reshape(BATCH, D)
    return (mixed_rows + ffn_out).astype(jnp.bfloat16)
```

```python
import functools
import math

import jax
import jax.numpy as jnp
from jax import lax
from jax.experimental import pallas as pl
from jax.experimental.pallas import tpu as pltpu
from jax.sharding import PartitionSpec as P

MESH = pl.DeviceIdType.MESH
F32 = jnp.float32
BF16 = jnp.bfloat16
LAG_ADD, LAG_HID, LAG_FWD, LAG_DOWN = 1, 5, 9, 11


def cuts(blocks, cap, cb):
    first = blocks - cap + cb
    mid = first + (cap - cb) // cb // 2 * cb
    edges = sorted({0, first, mid, blocks})
    return list(zip(edges[:-1], edges[1:]))


def layer_kernel(
    dims,
    lengths_ref,
    list_ref,
    count_ref,
    q_hbm,
    res_hbm,
    gain_hbm,
    k_hbm,
    v_hbm,
    gate_hbm,
    up_hbm,
    down_hbm,
    out_ref,
    q_ref,
    res_ref,
    gain_ref,
    k_vm,
    v_vm,
    down_vm,
    mixed,
    send_x,
    arrived,
    wide,
    x_vm,
    pair_out,
    pair_in,
    chip_out,
    chip_in,
    hid_all,
    acc,
    ret_out,
    ret_in,
    small_sem,
    kv_sem,
    w_sem,
    a2a_s,
    a2a_r,
    pair_s,
    pair_r,
    chip_s,
    chip_r,
    hid_s,
    hid_r,
    fwd_s,
    fwd_r,
    ret_s,
    ret_r,
    order_vm,
    order_sm,
    order_sem,
    *wide_w,
):
    n, mdl, rows, heads, hd, kv, cache, width, bw, cap, cb, blocks = dims
    parts_w = cuts(blocks, cap, cb)
    me = lax.axis_index("hid")
    group = me // mdl
    member = me % mdl
    base = group * mdl
    core = member % 2
    chip = member // 2
    chips = mdl // 2
    partner = base + chip * 2 + (1 - core)
    ds = width // mdl
    sub = ds // hd
    lanes = width // hd
    tile = rows * sub
    batch = rows * n
    rm = batch // mdl
    nch = cap // cb
    hpk = heads // kv
    step_blk = math.gcd(cb, blocks - cap)

    small = [
        pltpu.make_async_copy(src, dst, small_sem.at[i])
        for i, (src, dst) in enumerate(
            ((res_hbm, res_ref), (q_hbm, q_ref), (gain_hbm, gain_ref))
        )
    ]
    for copy in small:
        copy.start()
    kv_copies = []
    for r in range(rows):
        ck = pltpu.make_async_copy(k_hbm.at[r], k_vm.at[r], kv_sem.at[0, r])
        cv = pltpu.make_async_copy(v_hbm.at[r], v_vm.at[r], kv_sem.at[1, r])
        ck.start()
        cv.start()
        kv_copies.append((ck, cv))

    def start_weights():
        for at, (lo, hi) in enumerate(parts_w):
            for b in range(lo, hi, step_blk):
                for side_at, src in enumerate((gate_hbm, up_hbm)):
                    pltpu.make_async_copy(
                        src.at[0, pl.ds(b, step_blk)],
                        wide_w[at].at[pl.ds(b - lo, step_blk), side_at],
                        w_sem.at[at],
                    ).start()
        for b in range(0, blocks, step_blk):
            span = pl.ds(b, step_blk)
            pltpu.make_async_copy(down_hbm.at[0, span], down_vm.at[span], w_sem.at[3]).start()

    def weights_here(at):
        pltpu.make_async_copy(wide_w[at], wide_w[at], w_sem.at[at]).wait()

    barrier = pltpu.get_barrier_semaphore()

    def greet(d, carry):
        pl.semaphore_signal(
            barrier, inc=1, device_id={"hid": (me + d) % n}, device_id_type=MESH
        )
        return carry

    lax.fori_loop(1, n, greet, 0)

    side = -(-cap // 8) * 8
    lane = lax.broadcasted_iota(jnp.int32, (side, 128), 1)
    sub_at = lax.broadcasted_iota(jnp.int32, (side, 128), 0)
    listed = jnp.full((side, 128), blocks * 256, jnp.int32)
    for c in range(cap):
        listed = jnp.where(lane == c, list_ref[group, c] * 256 + c, listed)
    down_col = jnp.sum(jnp.where(lane == sub_at, listed, 0), axis=1, keepdims=True)
    rank = jnp.sum(jnp.where(listed < down_col, 1, 0), axis=1, keepdims=True)
    order_vm[...] = jnp.sum(
        jnp.where((rank == lane) & (sub_at < cap), down_col, 0), axis=0, keepdims=True
    )
    order_copy = pltpu.make_async_copy(order_vm, order_sm, order_sem)
    order_copy.start()

    for copy in small:
        copy.wait()
    for h in range(lanes):
        mixed[pl.ds(h, rows, stride=lanes), :] = res_ref[:, h * hd : (h + 1) * hd].astype(F32)

    slot = lax.broadcasted_iota(jnp.int32, (heads, cache), 1)
    q_rows = []
    for r in range(rows):
        q = q_ref[r].astype(F32)
        cols = []
        for k in range(kv):
            parts = []
            if k > 0:
                parts.append(jnp.zeros((k * hpk, hd), F32))
            parts.append(q[k * hpk : (k + 1) * hpk])
            if k < kv - 1:
                parts.append(jnp.zeros(((kv - 1 - k) * hpk, hd), F32))
            cols.append(jnp.concatenate(parts, axis=0).astype(BF16))
        q_rows.append(jnp.concatenate(cols, axis=1))
    for ck, cv in kv_copies:
        ck.wait()
        cv.wait()
    start_weights()
    order_copy.wait()
    scores = [
        lax.dot_general(
            q_rows[r], k_vm[r], (((1,), (1,)), ((), ())), preferred_element_type=F32
        ) * (1.0 / math.sqrt(hd))
        for r in range(rows)
    ]
    valid = [slot < lengths_ref[r] for r in range(rows)]
    scores = [jnp.where(valid[r], scores[r], -1e30) for r in range(rows)]
    tops = [jnp.max(v, axis=1, keepdims=True) for v in scores]
    terms = [jnp.where(valid[r], jnp.exp(scores[r] - tops[r]), 0.0) for r in range(rows)]
    sums = [jnp.sum(v, axis=1, keepdims=True) for v in terms]
    probs = [(terms[r] / sums[r]).astype(BF16) for r in range(rows)]
    mixed_rows = []
    for r in range(rows):
        wide_att = jnp.dot(probs[r], v_vm[r], preferred_element_type=F32)
        att = jnp.concatenate(
            [wide_att[k * hpk : (k + 1) * hpk, k * hd : (k + 1) * hd] for k in range(kv)], axis=0
        )
        mixed_rows.append(mixed[r * lanes : (r + 1) * lanes, :] + att)
    normed = []
    for r in range(rows):
        row = mixed_rows[r]
        mixed[r * lanes : (r + 1) * lanes, :] = row
        mean_sq = jnp.sum(jnp.sum(row * row, axis=1, keepdims=True), axis=0, keepdims=True) / width
        normed.append(row * lax.rsqrt(mean_sq + 1e-05) * gain_ref[...])
    for m in range(mdl):
        piece = jnp.concatenate([v[m * sub : (m + 1) * sub] for v in normed], axis=0)
        send_x[m] = piece.astype(BF16)

    pl.semaphore_wait(barrier, n - 1)

    def x_copy(d):
        to = (me + d) % n
        return pltpu.make_async_remote_copy(
            src_ref=send_x.at[to % mdl],
            dst_ref=arrived.at[me],
            send_sem=a2a_s.at[d],
            recv_sem=a2a_r.at[d],
            device_id={"hid": to},
            device_id_type=MESH,
        )

    def x_landed(d):
        return pltpu.make_async_remote_copy(
            src_ref=send_x.at[0],
            dst_ref=arrived.at[(me - d + n) % n],
            send_sem=a2a_s.at[d],
            recv_sem=a2a_r.at[d],
            device_id={"hid": (me - d + n) % n},
            device_id_type=MESH,
        )

    def loop(lo, hi, f):
        def body(i, carry):
            f(i)
            return carry

        lax.fori_loop(lo, hi, body, 0)

    loop(n // 2, n, lambda d: x_copy(d).start())
    loop(1, n // 2, lambda d: x_copy(d).start())
    arrived[me] = send_x[member]
    acc[...] = jnp.zeros_like(acc)
    loop(1, n, lambda d: x_landed(d).wait_recv())

    def widen(i):
        wide[pl.ds(pl.multiple_of(i * tile, tile), tile), :] = arrived[i].astype(F32)

    loop(0, n, widen)
    for j in range(sub):
        x_vm[:, j * hd : (j + 1) * hd] = wide[pl.ds(j, batch, stride=sub), :].astype(BF16)


    def remote(src, dst, ss, rs, to):
        return pltpu.make_async_remote_copy(
            src_ref=src, dst_ref=dst, send_sem=ss, recv_sem=rs,
            device_id={"hid": to}, device_id_type=MESH,
        )

    def pair_copy(i):
        return remote(
            pair_out.at[i, 1 - core], pair_in.at[i], pair_s.at[i], pair_r.at[i], partner
        )

    def chip_copy(i, k):
        to = (chip + k) % chips
        return remote(
            chip_out.at[i, to], chip_in.at[i, k - 1], chip_s.at[i, k - 1], chip_r.at[i, k - 1],
            base + to * 2 + core,
        )

    def hid_copy(i, k):
        to = partner if k == 0 else base + ((chip + k) % chips) * 2 + core
        return remote(
            hid_all.at[member, i], hid_all.at[member, i], hid_s.at[i, k], hid_r.at[i, k], to
        )

    def hid_landed(i, k):
        whose = chip * 2 + 1 - core if k == 0 else ((chip - k + chips) % chips) * 2 + core
        return remote(
            hid_all.at[whose, i], hid_all.at[whose, i], hid_s.at[i, k], hid_r.at[i, k], partner
        )

    def fwd_copy(i, k):
        whose = ((chip - k + chips) % chips) * 2 + core
        return remote(
            hid_all.at[whose, i], hid_all.at[whose, i], fwd_s.at[i, k - 1], fwd_r.at[i, k - 1],
            partner,
        )

    def fwd_landed(i, k):
        whose = ((chip - k + chips) % chips) * 2 + 1 - core
        return remote(
            hid_all.at[whose, i], hid_all.at[whose, i], fwd_s.at[i, k - 1], fwd_r.at[i, k - 1],
            partner,
        )

    def block_of(held, which):
        def one(at, side_at):
            lo, hi = parts_w[at]
            return wide_w[at][jnp.clip(which - lo, 0, hi - lo - 1), side_at]

        both = []
        for side_at in range(2):
            w = one(0, side_at)
            for at in range(1, held):
                w = jnp.where(which >= parts_w[at][0], one(at, side_at), w)
            both.append(w)
        return jnp.concatenate(both, axis=1)

    def project(i, held):
        x = x_vm[...]
        for pair in range(cb // 2):
            got = []
            for b in range(2):
                w = block_of(held, order_sm[0, i * cb + pair * 2 + b] // 256)
                got.append(jnp.dot(x, w, preferred_element_type=F32))
            for m in range(mdl):
                both = jnp.concatenate([y[m * rm : (m + 1) * rm] for y in got], axis=0)
                pair_out[i, m % 2, m // 2, pair * 2 * rm : (pair + 1) * 2 * rm, :] = both.astype(
                    BF16
                )
        pair_copy(i).start()

    def add_pair(i):
        pair_copy(i).wait_recv()
        for q in range(chips):
            total = pair_out[i, core, q].astype(F32) + pair_in[i, q].astype(F32)
            chip_out[i, q] = total.astype(BF16)
        for k in range(1, chips):
            chip_copy(i, k).start()

    def make_hidden(i):
        for k in range(1, chips):
            chip_copy(i, k).wait_recv()
        total = chip_out[i, chip].astype(F32)
        for k in range(1, chips):
            total = total + chip_in[i, k - 1].astype(F32)
        gate, up = total[:, :bw], total[:, bw:]
        row = lax.broadcasted_iota(jnp.int32, gate.shape, 0)
        active = row < 0
        for b in range(cb):
            live = order_sm[0, i * cb + b] % 256 < count_ref[group]
            active = active | ((row >= b * rm) & (row < jnp.where(live, (b + 1) * rm, 0)))
        hid_all[member, i] = jnp.where(active, jnp.maximum(gate, 0.0) * up, 0.0).astype(BF16)
        for k in range(1, chips):
            hid_copy(i, k).start()
        hid_copy(i, 0).start()

    def forward(i):
        for k in range(1, chips):
            hid_landed(i, k).wait_recv()
            fwd_copy(i, k).start()

    def down(i):
        hid_landed(i, 0).wait_recv()
        for k in range(1, chips):
            fwd_landed(i, k).wait_recv()
        total = acc[...]
        for pair in range(cb // 2):
            parts = []
            for m in range(mdl):
                two = hid_all[m, i, pair * 2 * rm : (pair + 1) * 2 * rm, :].astype(F32)
                parts.append(jnp.concatenate([two[:rm], two[rm:]], axis=1))
            lhs = jnp.concatenate(parts, axis=0).astype(BF16)
            w = jnp.concatenate(
                [down_vm[order_sm[0, i * cb + pair * 2 + b] // 256] for b in range(2)], axis=0
            )
            total = total + jnp.dot(lhs, w, preferred_element_type=F32)
        acc[...] = total

    def step(t):
        first = 0
        for at in range(len(parts_w)):
            last = (parts_w[at][1] - (blocks - cap)) // cb

            @pl.when(t == first)
            def _(at=at):
                weights_here(at)

            @pl.when((t >= first) & (t < last))
            def _(at=at):
                project(t, at + 1)

            first = last

        @pl.when((t >= LAG_ADD) & (t < nch + LAG_ADD))
        def _():
            add_pair(t - LAG_ADD)

        @pl.when((t >= LAG_HID) & (t < nch + LAG_HID))
        def _():
            make_hidden(t - LAG_HID)

        @pl.when((t >= LAG_FWD) & (t < nch + LAG_FWD))
        def _():
            forward(t - LAG_FWD)

        @pl.when(t == LAG_DOWN)
        def _():
            pltpu.make_async_copy(down_vm, down_vm, w_sem.at[3]).wait()

        @pl.when((t >= LAG_DOWN) & (t < nch + LAG_DOWN))
        def _():
            down(t - LAG_DOWN)

    loop(0, nch + LAG_DOWN, step)

    for j in range(sub):
        wide[pl.ds(j, batch, stride=sub), :] = acc[:, j * hd : (j + 1) * hd]

    def narrow(i):
        ret_out[i] = wide[pl.ds(pl.multiple_of(i * tile, tile), tile), :].astype(BF16)

    loop(0, n, narrow)

    def ret_copy(d):
        to = (me + d) % n
        return remote(ret_out.at[to], ret_in.at[me], ret_s.at[d], ret_r.at[d], to)

    def ret_landed(d):
        frm = (me - d + n) % n
        return remote(ret_out.at[0], ret_in.at[frm], ret_s.at[d], ret_r.at[d], frm)

    loop(n // 2, n, lambda d: ret_copy(d).start())
    loop(1, n // 2, lambda d: ret_copy(d).start())
    ret_in[me] = ret_out[me]

    def drain(i):
        pair_copy(i).wait_send()
        for k in range(1, chips):
            chip_copy(i, k).wait_send()
            fwd_copy(i, k).wait_send()
        for k in range(chips):
            hid_copy(i, k).wait_send()

    loop(0, nch, drain)
    loop(1, n, lambda d: x_copy(d).wait_send())
    loop(1, n, lambda d: ret_landed(d).wait_recv())
    for m in range(mdl):
        total = ret_in[m].astype(F32)
        for g in range(1, n // mdl):
            total = total + ret_in[g * mdl + m].astype(F32)
        for r in range(rows):
            at = r * lanes + m * sub
            mixed[at : at + sub, :] = mixed[at : at + sub, :] + total[r * sub : (r + 1) * sub]
    for h in range(lanes):
        out_ref[:, h * hd : (h + 1) * hd] = mixed[pl.ds(h, rows, stride=lanes), :].astype(BF16)
    loop(1, n, lambda d: ret_copy(d).wait_send())


def on_device(
    queries, k_cache, v_cache, lengths, residual_in, norm_gain,
    gate_w, up_w, down_w, block_list, block_count,
):
    n = lax.axis_size("hid")
    rows, heads, hd = queries.shape
    cache = k_cache.shape[1]
    kv = k_cache.shape[2] // hd
    width = residual_in.shape[1]
    _, blocks, ds, bw = gate_w.shape
    mdl = width // ds
    cap = block_list.shape[1]
    cb = 4 if cap % 4 == 0 else 2
    nch = cap // cb
    chips = mdl // 2
    batch = rows * n
    rm = batch // mdl
    sub = ds // hd
    tile = rows * sub
    dims = (n, mdl, rows, heads, hd, kv, cache, width, bw, cap, cb, blocks)
    dma = pltpu.SemaphoreType.DMA
    vmem = pl.BlockSpec(memory_space=pltpu.VMEM)
    smem = pl.BlockSpec(memory_space=pltpu.SMEM)
    hbm = pl.BlockSpec(memory_space=pl.ANY)
    return pl.pallas_call(
        functools.partial(layer_kernel, dims),
        out_shape=pltpu.VMEM((rows, width), BF16),
        in_specs=[smem] * 3 + [hbm] * 8,
        out_specs=vmem,
        scratch_shapes=[
            pltpu.VMEM(queries.shape, BF16),
            pltpu.VMEM(residual_in.shape, BF16),
            pltpu.VMEM((width // hd, hd), F32),
            pltpu.VMEM(k_cache.shape, BF16),
            pltpu.VMEM(v_cache.shape, BF16),
            pltpu.VMEM(down_w.shape[1:], BF16),
            pltpu.VMEM((rows * (width // hd), hd), F32),
            pltpu.VMEM((mdl, tile, hd), BF16),
            pltpu.VMEM((n, tile, hd), BF16),
            pltpu.VMEM((n * tile, hd), F32),
            pltpu.VMEM((batch, ds), BF16),
            pltpu.VMEM((nch, 2, chips, cb * rm, 2 * bw), BF16),
            pltpu.VMEM((nch, chips, cb * rm, 2 * bw), BF16),
            pltpu.VMEM((nch, chips, cb * rm, 2 * bw), BF16),
            pltpu.VMEM((nch, chips - 1, cb * rm, 2 * bw), BF16),
            pltpu.VMEM((mdl, nch, cb * rm, bw), BF16),
            pltpu.VMEM((batch, ds), F32),
            pltpu.VMEM((n, tile, hd), BF16),
            pltpu.VMEM((n, tile, hd), BF16),
            dma((3,)),
            dma((2, rows)),
            dma((4,)),
            dma((n,)),
            dma((n,)),
            dma((nch,)),
            dma((nch,)),
            dma((nch, chips - 1)),
            dma((nch, chips - 1)),
            dma((nch, chips)),
            dma((nch, chips)),
            dma((nch, chips - 1)),
            dma((nch, chips - 1)),
            dma((n,)),
            dma((n,)),
            pltpu.VMEM((1, 128), jnp.int32),
            pltpu.SMEM((1, 128), jnp.int32),
            dma(()),
        ]
        + [pltpu.VMEM((hi - lo, 2, ds, bw), BF16) for lo, hi in cuts(blocks, cap, cb)],
        compiler_params=pltpu.CompilerParams(
            collective_id=0, has_side_effects=True, vmem_limit_bytes=63_000_000
        ),
        name="decode_layer",
    )(
        lengths, block_list, block_count, queries, residual_in,
        norm_gain.reshape(width // hd, hd), k_cache, v_cache, gate_w, up_w, down_w,
    )


def solution(mesh):
    in_specs = (
        P(("groups", "hid"), None, None),
        P(("groups", "hid"), None, None),
        P(("groups", "hid"), None, None),
        P(("groups", "hid")),
        P(("groups", "hid"), None),
        P(),
        P("hid", None, None, None),
        P("hid", None, None, None),
        P("hid", None, None, None),
        P("groups", None),
        P("groups"),
    )
    out_specs = P(("groups", "hid"), None)
    return jax.shard_map(
        on_device, mesh=mesh, in_specs=in_specs, out_specs=out_specs, check_vma=False
    )
```

```python
import functools
import math

import jax
import jax.numpy as jnp
from jax import lax
from jax.experimental import pallas as pl
from jax.experimental.pallas import tpu as pltpu
from jax.sharding import PartitionSpec as P

MESH = pl.DeviceIdType.MESH
F32 = jnp.float32
BF16 = jnp.bfloat16
FAR, NEAR = 0, 1
KV_FIRST = 0
GATE_SETS, NEAR_SETS = (2, 4), (4,)
T_GATE_ADD = (-2, 2.0)
T_FAR_ADD = (4.5,)
T_NEAR_ADD = (11.6, 1)
T_FAR_HID = (20,)
T_NEAR_HID = (28.5, 0.1)
T_FAR_FWD = (30,)
T_FAR_DOWN = (34.5,)
T_NEAR_FWD = (37.9, 2)


def cut(count, edges):
    edges = [0, *(e for e in edges if e < count), count]
    return list(zip(edges[:-1], edges[1:]))


def layer_kernel(
    dims,
    lengths_ref,
    list_ref,
    count_ref,
    q_hbm,
    res_hbm,
    gain_hbm,
    k_hbm,
    v_hbm,
    gate_hbm,
    up_hbm,
    down_hbm,
    out_ref,
    q_ref,
    res_ref,
    gain_ref,
    kv_vm,
    gate_vm,
    up_vm,
    down_vm,
    mixed,
    send_x,
    arrived,
    wide,
    x_vm,
    pair_out,
    pair_in,
    chip_out,
    chip_in,
    hid_all,
    acc,
    ret_out,
    ret_in,
    small_sem,
    kv_sem,
    w_sem,
    x_s,
    x_r,
    pair_s,
    pair_r,
    chip_s,
    chip_r,
    hid_s,
    hid_r,
    fwd_s,
    fwd_r,
    ret_s,
    ret_r,
):
    n, mdl, rows, heads, hd, kv, cache, width, bw, cap, cb, blocks, groups = dims
    me = lax.axis_index("hid")
    group = me // mdl
    member = me % mdl
    base = group * mdl
    core = member % 2
    chip = member // 2
    chips = mdl // 2
    partner = base + chip * 2 + (1 - core)
    ds = width // mdl
    sub = ds // hd
    lanes = width // hd
    tile = rows * sub
    batch = rows * n
    nch = cap // cb
    hpk = heads // kv
    far_n = n - mdl
    part_rows = (rows * far_n, rows * mdl)
    part_at = (0, rows * far_n)
    rp = tuple(v // chips for v in part_rows)
    span = (pl.ds(0, 2 * rp[0]), pl.ds(2 * rp[0], 2 * rp[1]))
    step_blk = math.gcd(8, blocks)

    small = [
        pltpu.make_async_copy(src, dst, small_sem.at[i])
        for i, (src, dst) in enumerate(
            ((res_hbm, res_ref), (q_hbm, q_ref), (gain_hbm, gain_ref))
        )
    ]
    for copy in small:
        copy.start()
    for r in range(rows):
        pltpu.make_async_copy(k_hbm.at[r], kv_vm.at[r, 0], kv_sem.at[r]).start()
        pltpu.make_async_copy(v_hbm.at[r], kv_vm.at[r, 1], kv_sem.at[r]).start()

    def start_weights():
        for which, (src, vm) in enumerate(
            ((gate_hbm, gate_vm), (up_hbm, up_vm), (down_hbm, down_vm))
        ):
            for b in range(0, blocks, step_blk):
                at = pl.ds(b, step_blk)
                pltpu.make_async_copy(src.at[0, at], vm.at[at], w_sem.at[which]).start()

    def weights_here(which, vm):
        pltpu.make_async_copy(vm, vm, w_sem.at[which]).wait()

    barrier = pltpu.get_barrier_semaphore()

    def greet(d, carry):
        pl.semaphore_signal(
            barrier, inc=1, device_id={"hid": (me + d) % n}, device_id_type=MESH
        )
        return carry

    lax.fori_loop(1, n, greet, 0)

    for copy in small:
        copy.wait()
    for h in range(lanes):
        mixed[pl.ds(h, rows, stride=lanes), :] = res_ref[:, h * hd : (h + 1) * hd].astype(F32)

    slot = lax.broadcasted_iota(jnp.int32, (heads, cache), 1)
    q_rows = []
    for r in range(rows):
        q = q_ref[r].astype(F32)
        cols = []
        for k in range(kv):
            parts = []
            if k > 0:
                parts.append(jnp.zeros((k * hpk, hd), F32))
            parts.append(q[k * hpk : (k + 1) * hpk])
            if k < kv - 1:
                parts.append(jnp.zeros(((kv - 1 - k) * hpk, hd), F32))
            cols.append(jnp.concatenate(parts, axis=0).astype(BF16))
        q_rows.append(jnp.concatenate(cols, axis=1))
    for r in range(rows):
        if r == KV_FIRST:
            start_weights()
        pltpu.make_async_copy(kv_vm.at[r], kv_vm.at[r], kv_sem.at[r]).wait()
    scores = [
        lax.dot_general(
            q_rows[r], kv_vm[r, 0], (((1,), (1,)), ((), ())), preferred_element_type=F32
        ) * (1.0 / math.sqrt(hd))
        for r in range(rows)
    ]
    valid = [slot < lengths_ref[r] for r in range(rows)]
    scores = [jnp.where(valid[r], scores[r], -1e30) for r in range(rows)]
    tops = [jnp.max(v, axis=1, keepdims=True) for v in scores]
    terms = [jnp.where(valid[r], jnp.exp(scores[r] - tops[r]), 0.0) for r in range(rows)]
    sums = [jnp.sum(v, axis=1, keepdims=True) for v in terms]
    probs = [(terms[r] / sums[r]).astype(BF16) for r in range(rows)]
    mixed_rows = []
    for r in range(rows):
        wide_att = jnp.dot(probs[r], kv_vm[r, 1], preferred_element_type=F32)
        att = jnp.concatenate(
            [wide_att[k * hpk : (k + 1) * hpk, k * hd : (k + 1) * hd] for k in range(kv)],
            axis=0,
        )
        mixed_rows.append(mixed[r * lanes : (r + 1) * lanes, :] + att)
    normed = []
    for r in range(rows):
        row = mixed_rows[r]
        mixed[r * lanes : (r + 1) * lanes, :] = row
        mean_sq = (
            jnp.sum(jnp.sum(row * row, axis=1, keepdims=True), axis=0, keepdims=True) / width
        )
        normed.append(row * lax.rsqrt(mean_sq + 1e-05) * gain_ref[...])
    for m in range(mdl):
        piece = jnp.concatenate([v[m * sub : (m + 1) * sub] for v in normed], axis=0)
        send_x[m] = piece.astype(BF16)

    pl.semaphore_wait(barrier, n - 1)

    def remote(src, dst, ss, rs, to):
        return pltpu.make_async_remote_copy(
            src_ref=src, dst_ref=dst, send_sem=ss, recv_sem=rs,
            device_id={"hid": to}, device_id_type=MESH,
        )

    def landed(ref, sem):
        remote(ref, ref, x_s, sem, partner).wait_recv()

    def sent(ref, sem):
        remote(ref, ref, sem, ret_r.at[0], partner).wait_send()

    def loop(lo, hi, f):
        def body(i, carry):
            f(i)
            return carry

        lax.fori_loop(lo, hi, body, 0)

    def far_dev(k):
        return (group + 1 + k // mdl) % groups * mdl + (member + k % mdl) % mdl

    def near_dev(d):
        return base + (member + d) % mdl

    def x_copy(to, sem):
        return remote(send_x.at[to % mdl], arrived.at[me], x_s, sem, to)

    loop(0, far_n, lambda k: x_copy(far_dev(k), x_r.at[FAR]).start())
    loop(1, mdl, lambda d: x_copy(near_dev(d), x_r.at[NEAR]).start())
    arrived[me] = send_x[member]
    acc[...] = jnp.zeros_like(acc)

    def widen(at, src):
        wide[pl.ds(pl.multiple_of(at * tile, tile), tile), :] = arrived[src].astype(F32)

    landed(arrived.at[pl.ds(0, mdl - 1)], x_r.at[NEAR])
    loop(0, mdl, lambda m: widen(far_n + m, base + m))
    landed(arrived.at[pl.ds(0, far_n)], x_r.at[FAR])
    loop(0, far_n, lambda k: widen(k, (base + mdl + k) % n))
    for j in range(sub):
        x_vm[:, j * hd : (j + 1) * hd] = wide[pl.ds(j, batch, stride=sub), :].astype(BF16)
    weights_here(0, gate_vm)

    def pair_cols(vm, i, c):
        at = i * cb + c * 2
        return jnp.concatenate([vm[list_ref[group, at + b]] for b in range(2)], axis=1)

    def pack(y, s, i, c):
        for q in range(chips):
            for p in range(2):
                lo = part_at[p] + q * rp[p]
                y_q = y[lo : lo + rp[p]]
                pair_out[s, i, c, q, span[p], :] = jnp.concatenate(
                    [y_q[:, :bw], y_q[:, bw:]], axis=0
                ).astype(BF16)

    def gate_chunk(i):
        x = x_vm[...]
        for c in range(2):
            y = jnp.dot(x, pair_cols(gate_vm, i, c), preferred_element_type=F32)
            pack(y, 0, i, c)

    def up_chunk(i):
        x = x_vm[...]
        for c in range(2):
            y = jnp.dot(x, pair_cols(up_vm, i, c), preferred_element_type=F32)
            pack(y, 1, i, c)

    both = pl.ds(0, 2 * (rp[0] + rp[1]))

    def pair_copy(s, at, row, sem):
        return remote(
            pair_out.at[s, at, 1 - core, :, row], pair_in.at[s, at, :, row], pair_s, sem, partner
        )

    def add_pair(s, at, row):
        total = pair_out[s, at, core, :, row].astype(F32) + pair_in[s, at, :, row].astype(F32)
        chip_out[s, at, :, row] = total.astype(BF16)

    def chip_start(s, at, row, sem):
        for k in range(1, chips):
            to = (chip + k) % chips
            remote(
                chip_out.at[s, at, to, row], chip_in.at[s, at, k - 1, row], chip_s, sem,
                base + to * 2 + core,
            ).start()

    def total_of(s, i, row):
        total = chip_out[s, i, chip, row].astype(F32)
        for k in range(1, chips):
            total = total + chip_in[s, i, k - 1, row].astype(F32)
        return total

    def make_hidden(i, p):
        gate, up = total_of(0, i, span[p]), total_of(1, i, span[p])
        row = lax.broadcasted_iota(jnp.int32, gate.shape, 0)
        active = row < (count_ref[group] - (i * cb + core * 2)) * rp[p]
        hid_all[i, core, chip, span[p], :] = jnp.where(
            active, jnp.maximum(gate, 0.0) * up, 0.0
        ).astype(BF16)

    def hid_start(at, row, sem):
        for k in range(1, chips):
            to = (chip + k) % chips
            ref = hid_all.at[at, core, chip, row]
            remote(ref, ref, hid_s, sem, base + to * 2 + core).start()

    def hid_landed(at, row, sem):
        landed(hid_all.at[at, 0, pl.ds(0, chips - 1), row], sem)

    def fwd_copy(at, row, sem):
        ref = hid_all.at[at, core, :, row]
        return remote(ref, ref, fwd_s, sem, partner)

    def down(i, p):
        total = acc[pl.ds(part_at[p], part_rows[p]), :]
        for c in range(2):
            parts = []
            for q in range(chips):
                two = hid_all[i, c, q, span[p], :].astype(F32)
                parts.append(jnp.concatenate([two[: rp[p]], two[rp[p] :]], axis=1))
            lhs = jnp.concatenate(parts, axis=0).astype(BF16)
            w = jnp.concatenate(
                [down_vm[list_ref[group, i * cb + c * 2 + b]] for b in range(2)], axis=0
            )
            total = total + jnp.dot(lhs, w, preferred_element_type=F32)
        acc[pl.ds(part_at[p], part_rows[p]), :] = total

    gate_sets, near_sets = cut(nch, GATE_SETS), cut(nch, NEAR_SETS)
    G0, N0 = 0, len(gate_sets)
    C0 = N0 + len(near_sets)

    def ats(lo_hi):
        lo, hi = lo_hi
        return pl.ds(lo, hi - lo)

    def one(i):
        return pl.ds(i, 1)

    def gate_set(g):
        for i in range(*gate_sets[g]):
            gate_chunk(i)
        pair_copy(0, ats(gate_sets[g]), both, pair_r.at[G0 + g]).start()

    def gate_add(g):
        landed(pair_in.at[0, ats(gate_sets[g]), :, both], pair_r.at[G0 + g])
        loop(*gate_sets[g], lambda i: add_pair(0, i, both))
        chip_start(0, ats(gate_sets[g]), both, chip_r.at[G0 + g])

    def gate_land(g):
        landed(chip_in.at[0, ats(gate_sets[g]), :, both], chip_r.at[G0 + g])

    def far_up(i):
        up_chunk(i)
        pair_copy(1, one(i), span[FAR], pair_r.at[C0 + i]).start()

    def far_add(i):
        landed(pair_in.at[1, one(i), :, span[FAR]], pair_r.at[C0 + i])
        add_pair(1, i, span[FAR])
        chip_start(1, one(i), span[FAR], chip_r.at[C0 + i])

    def near_pair(g):
        pair_copy(1, ats(near_sets[g]), span[NEAR], pair_r.at[N0 + g]).start()

    def far_hidden(i):
        landed(chip_in.at[1, one(i), :, span[FAR]], chip_r.at[C0 + i])
        make_hidden(i, FAR)
        hid_start(one(i), span[FAR], hid_r.at[C0 + i])

    def far_forward(i):
        hid_landed(one(i), span[FAR], hid_r.at[C0 + i])
        fwd_copy(one(i), span[FAR], fwd_r.at[C0 + i]).start()

    def far_down(i):
        landed(hid_all.at[one(i), 0, :, span[FAR]], fwd_r.at[C0 + i])
        down(i, FAR)

    def near_add(g):
        landed(pair_in.at[1, ats(near_sets[g]), :, span[NEAR]], pair_r.at[N0 + g])
        loop(*near_sets[g], lambda i: add_pair(1, i, span[NEAR]))
        chip_start(1, ats(near_sets[g]), span[NEAR], chip_r.at[N0 + g])

    def near_hidden(g):
        landed(chip_in.at[1, ats(near_sets[g]), :, span[NEAR]], chip_r.at[N0 + g])
        loop(*near_sets[g], lambda i: make_hidden(i, NEAR))
        hid_start(ats(near_sets[g]), span[NEAR], hid_r.at[N0 + g])

    def near_forward(g):
        hid_landed(ats(near_sets[g]), span[NEAR], hid_r.at[N0 + g])
        fwd_copy(ats(near_sets[g]), span[NEAR], fwd_r.at[N0 + g]).start()

    def near_down(g):
        landed(hid_all.at[ats(near_sets[g]), 0, :, span[NEAR]], fwd_r.at[N0 + g])
        loop(*near_sets[g], lambda i: down(i, NEAR))

    def down_here(_):
        weights_here(2, down_vm)

    def narrow(k):
        ret_out[k] = wide[pl.ds(pl.multiple_of(k * tile, tile), tile), :].astype(BF16)

    def spread(p):
        for j in range(sub):
            wide[pl.ds(part_at[p] * sub + j, part_rows[p], stride=sub), :] = acc[
                pl.ds(part_at[p], part_rows[p]), j * hd : (j + 1) * hd
            ]

    def far_slot(k):
        to = far_dev(k)
        return (to - base - mdl + n) % n

    def far_return(_):
        spread(FAR)
        loop(0, far_n, narrow)
        loop(
            0,
            far_n,
            lambda k: remote(
                ret_out.at[far_slot(k)], ret_in.at[me], ret_s, ret_r.at[FAR], far_dev(k)
            ).start(),
        )

    def near_return(_):
        spread(NEAR)
        loop(far_n, n, narrow)
        loop(
            1,
            mdl,
            lambda d: remote(
                ret_out.at[far_n + (member + d) % mdl], ret_in.at[me], ret_s,
                ret_r.at[NEAR], near_dev(d),
            ).start(),
        )
        ret_in[me] = ret_out[far_n + member]

    ops = []

    def put(f, count, first, step=1.0):
        for i in range(count):
            ops.append((first + i * step, len(ops), f, i))

    ng, nn = len(gate_sets), len(near_sets)
    put(gate_set, ng, -20)
    put(gate_add, ng, *T_GATE_ADD)
    put(lambda _: weights_here(1, up_vm), 1, -0.5)
    put(far_up, nch, 0)
    for g, (lo, hi) in enumerate(near_sets):
        ops.append((hi - 0.9, len(ops), near_pair, g))
    put(far_add, nch, *T_FAR_ADD)
    put(near_add, nn, *T_NEAR_ADD)
    put(gate_land, ng, T_FAR_HID[0] - 0.5, 0.01)
    put(far_hidden, nch, *T_FAR_HID)
    put(near_hidden, nn, *T_NEAR_HID)
    put(far_forward, nch, *T_FAR_FWD)
    put(down_here, 1, T_FAR_DOWN[0] - 0.05)
    put(far_down, nch, *T_FAR_DOWN)
    end = max(t for t, *_ in ops)
    put(far_return, 1, end + 1)
    put(near_forward, nn, *T_NEAR_FWD)
    put(near_down, nn, end + 20)
    put(near_return, 1, end + 30)
    for _, _, f, i in sorted(ops, key=lambda v: v[:2]):
        f(i)

    sent(arrived.at[pl.ds(0, n - 1)], x_s)
    sent(pair_in, pair_s)
    sent(chip_in, chip_s)
    sent(hid_all.at[:, 0, pl.ds(0, chips - 1)], hid_s)
    sent(hid_all.at[:, 0], fwd_s)
    landed(ret_in.at[pl.ds(0, mdl - 1)], ret_r.at[NEAR])
    landed(ret_in.at[pl.ds(0, far_n)], ret_r.at[FAR])
    for m in range(mdl):
        total = ret_in[m].astype(F32)
        for g in range(1, groups):
            total = total + ret_in[g * mdl + m].astype(F32)
        for r in range(rows):
            at = r * lanes + m * sub
            mixed[at : at + sub, :] = mixed[at : at + sub, :] + total[r * sub : (r + 1) * sub]
    for h in range(lanes):
        out_ref[:, h * hd : (h + 1) * hd] = mixed[pl.ds(h, rows, stride=lanes), :].astype(BF16)
    sent(ret_in.at[pl.ds(0, n - 1)], ret_s)


def on_device(
    queries, k_cache, v_cache, lengths, residual_in, norm_gain,
    gate_w, up_w, down_w, block_list, block_count,
):
    n = lax.axis_size("hid")
    rows, heads, hd = queries.shape
    cache = k_cache.shape[1]
    kv = k_cache.shape[2] // hd
    width = residual_in.shape[1]
    _, blocks, ds, bw = gate_w.shape
    mdl = width // ds
    cap = block_list.shape[1]
    cb = 4
    nch = cap // cb
    chips = mdl // 2
    batch = rows * n
    sub = ds // hd
    tile = rows * sub
    groups = n // mdl
    piece = 2 * batch // chips
    marks = len(cut(nch, GATE_SETS)) + len(cut(nch, NEAR_SETS)) + nch
    dims = (n, mdl, rows, heads, hd, kv, cache, width, bw, cap, cb, blocks, groups)
    dma = pltpu.SemaphoreType.DMA
    vmem = pl.BlockSpec(memory_space=pltpu.VMEM)
    smem = pl.BlockSpec(memory_space=pltpu.SMEM)
    hbm = pl.BlockSpec(memory_space=pl.ANY)
    return pl.pallas_call(
        functools.partial(layer_kernel, dims),
        out_shape=pltpu.VMEM((rows, width), BF16),
        in_specs=[smem] * 3 + [hbm] * 8,
        out_specs=vmem,
        scratch_shapes=[
            pltpu.VMEM(queries.shape, BF16),
            pltpu.VMEM(residual_in.shape, BF16),
            pltpu.VMEM((width // hd, hd), F32),
            pltpu.VMEM((rows, 2, cache, kv * hd), BF16),
            pltpu.VMEM(gate_w.shape[1:], BF16),
            pltpu.VMEM(up_w.shape[1:], BF16),
            pltpu.VMEM(down_w.shape[1:], BF16),
            pltpu.VMEM((rows * (width // hd), hd), F32),
            pltpu.VMEM((mdl, tile, hd), BF16),
            pltpu.VMEM((n, tile, hd), BF16),
            pltpu.VMEM((n * tile, hd), F32),
            pltpu.VMEM((batch, ds), BF16),
            pltpu.VMEM((2, nch, 2, chips, piece, bw), BF16),
            pltpu.VMEM((2, nch, chips, piece, bw), BF16),
            pltpu.VMEM((2, nch, chips, piece, bw), BF16),
            pltpu.VMEM((2, nch, chips - 1, piece, bw), BF16),
            pltpu.VMEM((nch, 2, chips, piece, bw), BF16),
            pltpu.VMEM((batch, ds), F32),
            pltpu.VMEM((n, tile, hd), BF16),
            pltpu.VMEM((n, tile, hd), BF16),
            dma((3,)),
            dma((rows,)),
            dma((3,)),
            dma(()),
            dma((2,)),
            dma(()),
            dma((marks,)),
            dma(()),
            dma((marks,)),
            dma(()),
            dma((marks,)),
            dma(()),
            dma((marks,)),
            dma(()),
            dma((2,)),
        ],
        compiler_params=pltpu.CompilerParams(
            collective_id=0, has_side_effects=True, vmem_limit_bytes=63_000_000
        ),
        name="decode_layer",
    )(
        lengths, block_list, block_count, queries, residual_in,
        norm_gain.reshape(width // hd, hd), k_cache, v_cache, gate_w, up_w, down_w,
    )


def solution(mesh):
    in_specs = (
        P(("groups", "hid"), None, None),
        P(("groups", "hid"), None, None),
        P(("groups", "hid"), None, None),
        P(("groups", "hid")),
        P(("groups", "hid"), None),
        P(),
        P("hid", None, None, None),
        P("hid", None, None, None),
        P("hid", None, None, None),
        P("groups", None),
        P("groups"),
    )
    out_specs = P(("groups", "hid"), None)
    return jax.shard_map(
        on_device, mesh=mesh, in_specs=in_specs, out_specs=out_specs, check_vma=False
    )
```

```python
import functools
import math

import jax
import jax.numpy as jnp
from jax import lax
from jax.experimental import pallas as pl
from jax.experimental.pallas import tpu as pltpu
from jax.sharding import PartitionSpec as P

MESH = pl.DeviceIdType.MESH
F32 = jnp.float32
BF16 = jnp.bfloat16
FAR, NEAR = 0, 1
KV_FIRST = 0
EARLY = 1
DOWN_AT = 1
FARTHEST = True
GATE_WHOLE = True
GATE_SETS = (2, 4)
NEAR_SETS = (4,)
FAR_SETS = (1, 2, 3, 4, 5, 6)
DIRECT = ()
T_GATE_ADD = (-2, 1.2)
T_FAR_ADD = (4.5, 1)
T_NEAR_ADD = (11.6, 1)
T_FAR_HID = (20, 1)
T_NEAR_HID = (28.5, 0.1)
T_FAR_FWD = (30, 1)
T_FAR_DOWN = (34.5, 1)
T_NEAR_FWD = (37.9, 2)


def cut(count, edges):
    edges = [0, *(e for e in edges if e < count), count]
    return list(zip(edges[:-1], edges[1:]))


def layer_kernel(
    dims,
    lengths_hbm,
    list_hbm,
    count_hbm,
    q_hbm,
    res_hbm,
    gain_hbm,
    k_hbm,
    v_hbm,
    gate_hbm,
    up_hbm,
    down_hbm,
    out_ref,
    q_ref,
    res_ref,
    gain_ref,
    kv_vm,
    gate_vm,
    up_vm,
    down_vm,
    mixed,
    send_x,
    arrived,
    wide,
    x_vm,
    pair_out,
    pair_in,
    chip_out,
    chip_in,
    hid_all,
    acc,
    ret_out,
    ret_in,
    small_sem,
    kv_sem,
    w_sem,
    x_s,
    x_r,
    pair_s,
    pair_r,
    chip_s,
    chip_r,
    hid_s,
    hid_r,
    fwd_s,
    fwd_r,
    ret_s,
    ret_r,
    lengths_ref,
    list_ref,
    count_ref,
    tab_sem,
):
    n, mdl, rows, heads, hd, kv, cache, width, bw, cap, cb, blocks, groups = dims
    me = lax.axis_index("hid")
    group = me // mdl
    member = me % mdl
    base = group * mdl
    core = member % 2
    chip = member // 2
    chips = mdl // 2
    partner = base + chip * 2 + (1 - core)
    ds = width // mdl
    sub = ds // hd
    lanes = width // hd
    tile = rows * sub
    batch = rows * n
    nch = cap // cb
    quad = mdl // 2
    hpk = heads // kv
    far_n = n - mdl
    part_rows = (rows * far_n, rows * mdl)
    part_at = (0, rows * far_n)
    rp = tuple(v // chips for v in part_rows)
    span = (pl.ds(0, 2 * rp[0]), pl.ds(2 * rp[0], 2 * rp[1]))
    step_blk = math.gcd(8, blocks)

    small = [
        pltpu.make_async_copy(src, dst, small_sem.at[i])
        for i, (src, dst) in enumerate(
            ((res_hbm, res_ref), (q_hbm, q_ref), (gain_hbm, gain_ref))
        )
    ]
    for copy in small:
        copy.start()
    for r in range(rows):
        pltpu.make_async_copy(k_hbm.at[r], kv_vm.at[r, 0], kv_sem.at[r]).start()
        pltpu.make_async_copy(v_hbm.at[r], kv_vm.at[r, 1], kv_sem.at[r]).start()

    tables = [
        pltpu.make_async_copy(src, dst, tab_sem.at[i])
        for i, (src, dst) in enumerate(
            ((lengths_hbm, lengths_ref), (list_hbm, list_ref), (count_hbm, count_ref))
        )
    ]
    for copy in tables:
        copy.start()

    def start_weights(which, lo, hi):
        src, vm = ((gate_hbm, gate_vm), (up_hbm, up_vm), (down_hbm, down_vm))[which]
        for b in range(lo, hi, step_blk):
            at = pl.ds(b, step_blk)
            pltpu.make_async_copy(src.at[0, at], vm.at[at], w_sem.at[which]).start()

    def weights_here(which, vm):
        pltpu.make_async_copy(vm, vm, w_sem.at[which]).wait()

    early = min(EARLY * step_blk, blocks)
    start_weights(0, 0, early)
    barrier = pltpu.get_barrier_semaphore()

    def greet(d, carry):
        pl.semaphore_signal(
            barrier, inc=1, device_id={"hid": (me + d) % n}, device_id_type=MESH
        )
        return carry

    lax.fori_loop(1, n, greet, 0)

    for copy in small:
        copy.wait()
    for copy in tables:
        copy.wait()
    for h in range(lanes):
        mixed[pl.ds(h, rows, stride=lanes), :] = res_ref[:, h * hd : (h + 1) * hd].astype(F32)

    slot = lax.broadcasted_iota(jnp.int32, (heads, cache), 1)
    q_rows = []
    for r in range(rows):
        q = q_ref[r].astype(F32)
        cols = []
        for k in range(kv):
            parts = []
            if k > 0:
                parts.append(jnp.zeros((k * hpk, hd), F32))
            parts.append(q[k * hpk : (k + 1) * hpk])
            if k < kv - 1:
                parts.append(jnp.zeros(((kv - 1 - k) * hpk, hd), F32))
            cols.append(jnp.concatenate(parts, axis=0).astype(BF16))
        q_rows.append(jnp.concatenate(cols, axis=1))
    for r in range(rows):
        if r == KV_FIRST:
            start_weights(0, early, blocks)
            start_weights(1, 0, blocks)
            if DOWN_AT == 0:
                start_weights(2, 0, blocks)
        pltpu.make_async_copy(kv_vm.at[r], kv_vm.at[r], kv_sem.at[r]).wait()
    scores = [
        lax.dot_general(
            q_rows[r], kv_vm[r, 0], (((1,), (1,)), ((), ())), preferred_element_type=F32
        ) * (1.0 / math.sqrt(hd))
        for r in range(rows)
    ]
    valid = [slot < lengths_ref[r] for r in range(rows)]
    scores = [jnp.where(valid[r], scores[r], -1e30) for r in range(rows)]
    tops = [jnp.max(v, axis=1, keepdims=True) for v in scores]
    terms = [jnp.where(valid[r], jnp.exp(scores[r] - tops[r]), 0.0) for r in range(rows)]
    sums = [jnp.sum(v, axis=1, keepdims=True) for v in terms]
    probs = [(terms[r] / sums[r]).astype(BF16) for r in range(rows)]
    mixed_rows = []
    for r in range(rows):
        wide_att = jnp.dot(probs[r], kv_vm[r, 1], preferred_element_type=F32)
        att = jnp.concatenate(
            [wide_att[k * hpk : (k + 1) * hpk, k * hd : (k + 1) * hd] for k in range(kv)],
            axis=0,
        )
        mixed_rows.append(mixed[r * lanes : (r + 1) * lanes, :] + att)
    normed = []
    for r in range(rows):
        row = mixed_rows[r]
        mixed[r * lanes : (r + 1) * lanes, :] = row
        mean_sq = (
            jnp.sum(jnp.sum(row * row, axis=1, keepdims=True), axis=0, keepdims=True) / width
        )
        normed.append(row * lax.rsqrt(mean_sq + 1e-05) * gain_ref[...])
    for m in range(mdl):
        piece = jnp.concatenate([v[m * sub : (m + 1) * sub] for v in normed], axis=0)
        send_x[m] = piece.astype(BF16)

    pl.semaphore_wait(barrier, n - 1)

    def remote(src, dst, ss, rs, to):
        return pltpu.make_async_remote_copy(
            src_ref=src, dst_ref=dst, send_sem=ss, recv_sem=rs,
            device_id={"hid": to}, device_id_type=MESH,
        )

    def landed(ref, sem):
        remote(ref, ref, x_s, sem, partner).wait_recv()

    def sent(ref, sem):
        remote(ref, ref, sem, ret_r.at[0], partner).wait_send()

    def loop(lo, hi, f):
        def body(i, carry):
            f(i)
            return carry

        lax.fori_loop(lo, hi, body, 0)

    def far_dev(k):
        ahead, way = k // mdl, k % mdl
        turn = (way // quad + 1 + group) % 2 * quad + (member + way) % quad
        return (group + 1 + ahead) % groups * mdl + (turn if FARTHEST else (member + way) % mdl)

    def near_dev(d):
        return base + (member + d) % mdl

    def x_copy(to, sem):
        return remote(send_x.at[to % mdl], arrived.at[me], x_s, sem, to)

    loop(0, far_n, lambda k: x_copy(far_dev(k), x_r.at[FAR]).start())
    loop(1, mdl, lambda d: x_copy(near_dev(d), x_r.at[NEAR]).start())
    arrived[me] = send_x[member]
    acc[...] = jnp.zeros_like(acc)

    def widen(at, src):
        wide[pl.ds(pl.multiple_of(at * tile, tile), tile), :] = arrived[src].astype(F32)

    if DOWN_AT == 1:
        start_weights(2, 0, blocks)
    landed(arrived.at[pl.ds(0, mdl - 1)], x_r.at[NEAR])
    loop(0, mdl, lambda m: widen(far_n + m, base + m))
    landed(arrived.at[pl.ds(0, far_n)], x_r.at[FAR])
    if DOWN_AT == 2:
        start_weights(2, 0, blocks)
    loop(0, far_n, lambda k: widen(k, (base + mdl + k) % n))
    for j in range(sub):
        x_vm[:, j * hd : (j + 1) * hd] = wide[pl.ds(j, batch, stride=sub), :].astype(BF16)
    weights_here(0, gate_vm)

    def pair_cols(vm, i, c):
        at = i * cb + c * 2
        return jnp.concatenate([vm[list_ref[group, at + b]] for b in range(2)], axis=1)

    def pack(y, s, i, c):
        for q in range(chips):
            for p in range(2):
                lo = part_at[p] + q * rp[p]
                y_q = y[lo : lo + rp[p]]
                pair_out[s, i, c, q, span[p], :] = jnp.concatenate(
                    [y_q[:, :bw], y_q[:, bw:]], axis=0
                ).astype(BF16)

    def gate_chunk(i):
        x = x_vm[...]
        for c in range(2):
            y = jnp.dot(x, pair_cols(gate_vm, i, c), preferred_element_type=F32)
            pack(y, 0, i, c)

    def up_chunk(i):
        x = x_vm[...]
        for c in range(2):
            y = jnp.dot(x, pair_cols(up_vm, i, c), preferred_element_type=F32)
            pack(y, 1, i, c)

    both = pl.ds(0, 2 * (rp[0] + rp[1]))

    def pair_copy(s, at, row, sem):
        return remote(
            pair_out.at[s, at, 1 - core, :, row], pair_in.at[s, at, :, row], pair_s, sem, partner
        )

    def add_pair(s, at, row):
        total = pair_out[s, at, core, :, row].astype(F32) + pair_in[s, at, :, row].astype(F32)
        chip_out[s, at, :, row] = total.astype(BF16)

    def chip_start(s, at, row, sem):
        for k in range(1, chips):
            to = (chip + k) % chips
            remote(
                chip_out.at[s, at, to, row], chip_in.at[s, at, k - 1, row], chip_s, sem,
                base + to * 2 + core,
            ).start()

    def total_of(s, i, row):
        total = chip_out[s, i, chip, row].astype(F32)
        for k in range(1, chips):
            total = total + chip_in[s, i, k - 1, row].astype(F32)
        return total

    def make_hidden(i, p):
        gate, up = total_of(0, i, span[p]), total_of(1, i, span[p])
        row = lax.broadcasted_iota(jnp.int32, gate.shape, 0)
        active = row < (count_ref[group] - (i * cb + core * 2)) * rp[p]
        hid_all[i, core, chip, span[p], :] = jnp.where(
            active, jnp.maximum(gate, 0.0) * up, 0.0
        ).astype(BF16)

    def hid_start(at, row, sem):
        for k in range(1, chips):
            to = (chip + k) % chips
            ref = hid_all.at[at, core, chip, row]
            remote(ref, ref, hid_s, sem, base + to * 2 + core).start()

    def cross_start(at, row, sem):
        for k in range(chips):
            to = (chip + (k + 1) % chips) % chips
            ref = hid_all.at[at, core, chip, row]
            remote(ref, ref, fwd_s, sem, base + to * 2 + (1 - core)).start()

    def hid_landed(at, row, sem):
        landed(hid_all.at[at, 0, pl.ds(0, chips - 1), row], sem)

    def fwd_copy(at, row, sem):
        ref = hid_all.at[at, core, :, row]
        return remote(ref, ref, fwd_s, sem, partner)

    def down(i, p):
        total = acc[pl.ds(part_at[p], part_rows[p]), :]
        for c in range(2):
            parts = []
            for q in range(chips):
                two = hid_all[i, c, q, span[p], :].astype(F32)
                parts.append(jnp.concatenate([two[: rp[p]], two[rp[p] :]], axis=1))
            lhs = jnp.concatenate(parts, axis=0).astype(BF16)
            w = jnp.concatenate(
                [down_vm[list_ref[group, i * cb + c * 2 + b]] for b in range(2)], axis=0
            )
            total = total + jnp.dot(lhs, w, preferred_element_type=F32)
        acc[pl.ds(part_at[p], part_rows[p]), :] = total

    gate_sets, near_sets = cut(nch, GATE_SETS), cut(nch, NEAR_SETS)
    G0, N0 = 0, len(gate_sets)
    far_sets = cut(nch, FAR_SETS)
    C0 = N0 + len(near_sets)

    def ats(lo_hi):
        lo, hi = lo_hi
        return pl.ds(lo, hi - lo)

    def gate_set(g):
        for i in range(*gate_sets[g]):
            gate_chunk(i)
        pair_copy(0, ats(gate_sets[g]), both, pair_r.at[G0 + g]).start()

    def gate_add(g):
        landed(pair_in.at[0, ats(gate_sets[g]), :, both], pair_r.at[G0 + g])
        loop(*gate_sets[g], lambda i: add_pair(0, i, both))
        if GATE_WHOLE:
            chip_start(0, ats(gate_sets[g]), both, chip_r.at[G0 + g])
        else:
            chip_start(0, ats(gate_sets[g]), span[FAR], chip_r.at[G0 + g])
            chip_start(0, ats(gate_sets[g]), span[NEAR], chip_r.at[G0 + g])

    def gate_land(g):
        landed(chip_in.at[0, ats(gate_sets[g]), :, both], chip_r.at[G0 + g])

    def far_up(g):
        for i in range(*far_sets[g]):
            up_chunk(i)
        pair_copy(1, ats(far_sets[g]), span[FAR], pair_r.at[C0 + g]).start()

    def far_add(g):
        landed(pair_in.at[1, ats(far_sets[g]), :, span[FAR]], pair_r.at[C0 + g])
        for i in range(*far_sets[g]):
            add_pair(1, i, span[FAR])
        chip_start(1, ats(far_sets[g]), span[FAR], chip_r.at[C0 + g])

    def near_pair(g):
        pair_copy(1, ats(near_sets[g]), span[NEAR], pair_r.at[N0 + g]).start()

    def far_hidden(g):
        at = ats(far_sets[g])
        landed(chip_in.at[1, at, :, span[FAR]], chip_r.at[C0 + g])
        for i in range(*far_sets[g]):
            make_hidden(i, FAR)
        hid_start(at, span[FAR], hid_r.at[C0 + g])
        if g in DIRECT:
            cross_start(at, span[FAR], fwd_r.at[C0 + g])

    def far_forward(g):
        hid_landed(ats(far_sets[g]), span[FAR], hid_r.at[C0 + g])
        if g not in DIRECT:
            fwd_copy(ats(far_sets[g]), span[FAR], fwd_r.at[C0 + g]).start()

    def far_down(g):
        landed(hid_all.at[ats(far_sets[g]), 0, :, span[FAR]], fwd_r.at[C0 + g])
        for i in range(*far_sets[g]):
            down(i, FAR)

    def near_add(g):
        landed(pair_in.at[1, ats(near_sets[g]), :, span[NEAR]], pair_r.at[N0 + g])
        loop(*near_sets[g], lambda i: add_pair(1, i, span[NEAR]))
        chip_start(1, ats(near_sets[g]), span[NEAR], chip_r.at[N0 + g])

    def near_hidden(g):
        landed(chip_in.at[1, ats(near_sets[g]), :, span[NEAR]], chip_r.at[N0 + g])
        loop(*near_sets[g], lambda i: make_hidden(i, NEAR))
        hid_start(ats(near_sets[g]), span[NEAR], hid_r.at[N0 + g])

    def near_forward(g):
        hid_landed(ats(near_sets[g]), span[NEAR], hid_r.at[N0 + g])
        fwd_copy(ats(near_sets[g]), span[NEAR], fwd_r.at[N0 + g]).start()

    def near_down(g):
        landed(hid_all.at[ats(near_sets[g]), 0, :, span[NEAR]], fwd_r.at[N0 + g])
        loop(*near_sets[g], lambda i: down(i, NEAR))

    def down_here(_):
        weights_here(2, down_vm)

    def narrow(k):
        ret_out[k] = wide[pl.ds(pl.multiple_of(k * tile, tile), tile), :].astype(BF16)

    def spread(p):
        for j in range(sub):
            wide[pl.ds(part_at[p] * sub + j, part_rows[p], stride=sub), :] = acc[
                pl.ds(part_at[p], part_rows[p]), j * hd : (j + 1) * hd
            ]

    def far_slot(k):
        to = far_dev(k)
        return (to - base - mdl + n) % n

    def far_return(_):
        spread(FAR)
        loop(0, far_n, narrow)
        loop(
            0,
            far_n,
            lambda k: remote(
                ret_out.at[far_slot(k)], ret_in.at[me], ret_s, ret_r.at[FAR], far_dev(k)
            ).start(),
        )

    def near_return(_):
        spread(NEAR)
        loop(far_n, n, narrow)
        loop(
            1,
            mdl,
            lambda d: remote(
                ret_out.at[far_n + (member + d) % mdl], ret_in.at[me], ret_s,
                ret_r.at[NEAR], near_dev(d),
            ).start(),
        )
        ret_in[me] = ret_out[far_n + member]

    ops = []

    def put(f, count, first, step=1.0):
        for i in range(count):
            ops.append((first + i * step, len(ops), f, i))

    ng, nn, nf = len(gate_sets), len(near_sets), len(far_sets)
    put(gate_set, ng, -20)
    put(gate_add, ng, *T_GATE_ADD)
    put(lambda _: weights_here(1, up_vm), 1, -0.5)
    if DOWN_AT == 3:
        put(lambda _: start_weights(2, 0, blocks), 1, -3)
    for g, (lo, hi) in enumerate(far_sets):
        ops.append((hi - 1.0, len(ops), far_up, g))
    for g, (lo, hi) in enumerate(near_sets):
        ops.append((nch - 0.9, len(ops), near_pair, g))
    put(far_add, nf, *T_FAR_ADD)
    put(near_add, nn, *T_NEAR_ADD)
    put(gate_land, ng, T_FAR_HID[0] - 0.5, 0.01)
    put(far_hidden, nf, *T_FAR_HID)
    put(near_hidden, nn, *T_NEAR_HID)
    put(far_forward, nf, *T_FAR_FWD)
    put(down_here, 1, T_FAR_DOWN[0] - 0.05)
    put(far_down, nf, *T_FAR_DOWN)
    end = max(t for t, *_ in ops)
    put(far_return, 1, end + 1)
    put(near_forward, nn, *T_NEAR_FWD)
    put(near_down, nn, end + 20)
    put(near_return, 1, end + 30)
    for _, _, f, i in sorted(ops, key=lambda v: v[:2]):
        f(i)

    sent(arrived.at[pl.ds(0, n - 1)], x_s)
    sent(pair_in, pair_s)
    sent(chip_in, chip_s)
    sent(hid_all.at[:, 0, pl.ds(0, chips - 1)], hid_s)
    sent(hid_all.at[:, 0], fwd_s)
    landed(ret_in.at[pl.ds(0, mdl - 1)], ret_r.at[NEAR])
    landed(ret_in.at[pl.ds(0, far_n)], ret_r.at[FAR])
    for m in range(mdl):
        total = ret_in[m].astype(F32)
        for g in range(1, groups):
            total = total + ret_in[g * mdl + m].astype(F32)
        for r in range(rows):
            at = r * lanes + m * sub
            mixed[at : at + sub, :] = mixed[at : at + sub, :] + total[r * sub : (r + 1) * sub]
    for h in range(lanes):
        out_ref[:, h * hd : (h + 1) * hd] = mixed[pl.ds(h, rows, stride=lanes), :].astype(BF16)
    sent(ret_in.at[pl.ds(0, n - 1)], ret_s)


def on_device(
    queries, k_cache, v_cache, lengths, residual_in, norm_gain,
    gate_w, up_w, down_w, block_list, block_count,
):
    n = lax.axis_size("hid")
    rows, heads, hd = queries.shape
    cache = k_cache.shape[1]
    kv = k_cache.shape[2] // hd
    width = residual_in.shape[1]
    _, blocks, ds, bw = gate_w.shape
    mdl = width // ds
    cap = block_list.shape[1]
    cb = 4
    nch = cap // cb
    chips = mdl // 2
    batch = rows * n
    sub = ds // hd
    tile = rows * sub
    groups = n // mdl
    piece = 2 * batch // chips
    marks = len(cut(nch, GATE_SETS)) + len(cut(nch, NEAR_SETS)) + len(cut(nch, FAR_SETS))
    dims = (n, mdl, rows, heads, hd, kv, cache, width, bw, cap, cb, blocks, groups)
    dma = pltpu.SemaphoreType.DMA
    vmem = pl.BlockSpec(memory_space=pltpu.VMEM)
    hbm = pl.BlockSpec(memory_space=pl.ANY)
    return pl.pallas_call(
        functools.partial(layer_kernel, dims),
        out_shape=pltpu.VMEM((rows, width), BF16),
        in_specs=[hbm] * 11,
        out_specs=vmem,
        scratch_shapes=[
            pltpu.VMEM(queries.shape, BF16),
            pltpu.VMEM(residual_in.shape, BF16),
            pltpu.VMEM((width // hd, hd), F32),
            pltpu.VMEM((rows, 2, cache, kv * hd), BF16),
            pltpu.VMEM(gate_w.shape[1:], BF16),
            pltpu.VMEM(up_w.shape[1:], BF16),
            pltpu.VMEM(down_w.shape[1:], BF16),
            pltpu.VMEM((rows * (width // hd), hd), F32),
            pltpu.VMEM((mdl, tile, hd), BF16),
            pltpu.VMEM((n, tile, hd), BF16),
            pltpu.VMEM((n * tile, hd), F32),
            pltpu.VMEM((batch, ds), BF16),
            pltpu.VMEM((2, nch, 2, chips, piece, bw), BF16),
            pltpu.VMEM((2, nch, chips, piece, bw), BF16),
            pltpu.VMEM((2, nch, chips, piece, bw), BF16),
            pltpu.VMEM((2, nch, chips - 1, piece, bw), BF16),
            pltpu.VMEM((nch, 2, chips, piece, bw), BF16),
            pltpu.VMEM((batch, ds), F32),
            pltpu.VMEM((n, tile, hd), BF16),
            pltpu.VMEM((n, tile, hd), BF16),
            dma((3,)),
            dma((rows,)),
            dma((3,)),
            dma(()),
            dma((2,)),
            dma(()),
            dma((marks,)),
            dma(()),
            dma((marks,)),
            dma(()),
            dma((marks,)),
            dma(()),
            dma((marks,)),
            dma(()),
            dma((2,)),
            pltpu.SMEM(lengths.shape, jnp.int32),
            pltpu.SMEM(block_list.shape, jnp.int32),
            pltpu.SMEM(block_count.shape, jnp.int32),
            dma((3,)),
        ],
        compiler_params=pltpu.CompilerParams(
            collective_id=0, has_side_effects=True, vmem_limit_bytes=63_000_000
        ),
        name="decode_layer",
    )(
        lengths, block_list, block_count, queries, residual_in,
        norm_gain.reshape(width // hd, hd), k_cache, v_cache, gate_w, up_w, down_w,
    )


def solution(mesh):
    in_specs = (
        P(("groups", "hid"), None, None),
        P(("groups", "hid"), None, None),
        P(("groups", "hid"), None, None),
        P(("groups", "hid")),
        P(("groups", "hid"), None),
        P(),
        P("hid", None, None, None),
        P("hid", None, None, None),
        P("hid", None, None, None),
        P("groups", None),
        P("groups"),
    )
    out_specs = P(("groups", "hid"), None)
    return jax.shard_map(
        on_device, mesh=mesh, in_specs=in_specs, out_specs=out_specs, check_vma=False
    )
```

```python
import functools
import math

import jax
import jax.numpy as jnp
from jax import lax
from jax.experimental import pallas as pl
from jax.experimental.pallas import tpu as pltpu
from jax.sharding import PartitionSpec as P

MESH = pl.DeviceIdType.MESH
F32 = jnp.float32
BF16 = jnp.bfloat16
FAR, NEAR = 0, 1
KV_FIRST = 0
EARLY = 1
DOWN_AT = 1
FARTHEST = True
GATE_WHOLE = True
GATE_SETS = (2, 4)
NEAR_SETS = ()
FAR_SETS = (1, 2, 3, 4, 5, 6)
JOINT = 4
DIRECT = ()
T_GATE_ADD = (-2, 1.2)
T_FAR_ADD = (4.5, 1)
T_NEAR_ADD = (11.6, 1)
T_FAR_HID = (20, 1)
T_NEAR_HID = (28.5, 0.1)
T_FAR_FWD = (30, 1)
T_FAR_DOWN = (34.5, 1)
T_NEAR_FWD = (37.9, 2)


def near_cut(count):
    lo = max([hi for _, hi in cut(count, FAR_SETS) if hi <= JOINT], default=0)
    edges = [lo, *(e for e in NEAR_SETS if lo < e < count), count]
    return [(a, b) for a, b in zip(edges[:-1], edges[1:]) if b > a]


def cut(count, edges):
    edges = [0, *(e for e in edges if e < count), count]
    return list(zip(edges[:-1], edges[1:]))


def layer_kernel(
    dims,
    lengths_hbm,
    list_hbm,
    count_hbm,
    q_hbm,
    res_hbm,
    gain_hbm,
    k_hbm,
    v_hbm,
    gate_hbm,
    up_hbm,
    down_hbm,
    out_ref,
    q_ref,
    res_ref,
    gain_ref,
    kv_vm,
    gate_vm,
    up_vm,
    down_vm,
    mixed,
    send_x,
    arrived,
    wide,
    x_vm,
    pair_out,
    pair_in,
    chip_out,
    chip_in,
    hid_all,
    acc,
    ret_out,
    ret_in,
    small_sem,
    kv_sem,
    w_sem,
    x_s,
    x_r,
    pair_s,
    pair_r,
    chip_s,
    chip_r,
    hid_s,
    hid_r,
    fwd_s,
    fwd_r,
    ret_s,
    ret_r,
    lengths_ref,
    list_ref,
    count_ref,
    tab_sem,
):
    n, mdl, rows, heads, hd, kv, cache, width, bw, cap, cb, blocks, groups = dims
    me = lax.axis_index("hid")
    group = me // mdl
    member = me % mdl
    base = group * mdl
    core = member % 2
    chip = member // 2
    chips = mdl // 2
    partner = base + chip * 2 + (1 - core)
    ds = width // mdl
    sub = ds // hd
    lanes = width // hd
    tile = rows * sub
    batch = rows * n
    nch = cap // cb
    quad = mdl // 2
    hpk = heads // kv
    far_n = n - mdl
    part_rows = (rows * far_n, rows * mdl)
    part_at = (0, rows * far_n)
    rp = tuple(v // chips for v in part_rows)
    span = (pl.ds(0, 2 * rp[0]), pl.ds(2 * rp[0], 2 * rp[1]))
    step_blk = math.gcd(8, blocks)

    small = [
        pltpu.make_async_copy(src, dst, small_sem.at[i])
        for i, (src, dst) in enumerate(
            ((res_hbm, res_ref), (q_hbm, q_ref), (gain_hbm, gain_ref))
        )
    ]
    for copy in small:
        copy.start()
    for r in range(rows):
        pltpu.make_async_copy(k_hbm.at[r], kv_vm.at[r, 0], kv_sem.at[r]).start()
        pltpu.make_async_copy(v_hbm.at[r], kv_vm.at[r, 1], kv_sem.at[r]).start()

    tables = [
        pltpu.make_async_copy(src, dst, tab_sem.at[i])
        for i, (src, dst) in enumerate(
            ((lengths_hbm, lengths_ref), (list_hbm, list_ref), (count_hbm, count_ref))
        )
    ]
    for copy in tables:
        copy.start()

    def start_weights(which, lo, hi):
        src, vm = ((gate_hbm, gate_vm), (up_hbm, up_vm), (down_hbm, down_vm))[which]
        for b in range(lo, hi, step_blk):
            at = pl.ds(b, step_blk)
            pltpu.make_async_copy(src.at[0, at], vm.at[at], w_sem.at[which]).start()

    def weights_here(which, vm):
        pltpu.make_async_copy(vm, vm, w_sem.at[which]).wait()

    early = min(EARLY * step_blk, blocks)
    start_weights(0, 0, early)
    barrier = pltpu.get_barrier_semaphore()

    def greet(d, carry):
        pl.semaphore_signal(
            barrier, inc=1, device_id={"hid": (me + d) % n}, device_id_type=MESH
        )
        return carry

    lax.fori_loop(1, n, greet, 0)

    for copy in small:
        copy.wait()
    for copy in tables:
        copy.wait()
    for h in range(lanes):
        mixed[pl.ds(h, rows, stride=lanes), :] = res_ref[:, h * hd : (h + 1) * hd].astype(F32)

    slot = lax.broadcasted_iota(jnp.int32, (heads, cache), 1)
    q_rows = []
    for r in range(rows):
        q = q_ref[r].astype(F32)
        cols = []
        for k in range(kv):
            parts = []
            if k > 0:
                parts.append(jnp.zeros((k * hpk, hd), F32))
            parts.append(q[k * hpk : (k + 1) * hpk])
            if k < kv - 1:
                parts.append(jnp.zeros(((kv - 1 - k) * hpk, hd), F32))
            cols.append(jnp.concatenate(parts, axis=0).astype(BF16))
        q_rows.append(jnp.concatenate(cols, axis=1))
    for r in range(rows):
        if r == KV_FIRST:
            start_weights(0, early, blocks)
            start_weights(1, 0, blocks)
            if DOWN_AT == 0:
                start_weights(2, 0, blocks)
        pltpu.make_async_copy(kv_vm.at[r], kv_vm.at[r], kv_sem.at[r]).wait()
    scores = [
        lax.dot_general(
            q_rows[r], kv_vm[r, 0], (((1,), (1,)), ((), ())), preferred_element_type=F32
        ) * (1.0 / math.sqrt(hd))
        for r in range(rows)
    ]
    valid = [slot < lengths_ref[r] for r in range(rows)]
    scores = [jnp.where(valid[r], scores[r], -1e30) for r in range(rows)]
    tops = [jnp.max(v, axis=1, keepdims=True) for v in scores]
    terms = [jnp.where(valid[r], jnp.exp(scores[r] - tops[r]), 0.0) for r in range(rows)]
    sums = [jnp.sum(v, axis=1, keepdims=True) for v in terms]
    probs = [(terms[r] / sums[r]).astype(BF16) for r in range(rows)]
    mixed_rows = []
    for r in range(rows):
        wide_att = jnp.dot(probs[r], kv_vm[r, 1], preferred_element_type=F32)
        att = jnp.concatenate(
            [wide_att[k * hpk : (k + 1) * hpk, k * hd : (k + 1) * hd] for k in range(kv)],
            axis=0,
        )
        mixed_rows.append(mixed[r * lanes : (r + 1) * lanes, :] + att)
    normed = []
    for r in range(rows):
        row = mixed_rows[r]
        mixed[r * lanes : (r + 1) * lanes, :] = row
        mean_sq = (
            jnp.sum(jnp.sum(row * row, axis=1, keepdims=True), axis=0, keepdims=True) / width
        )
        normed.append(row * lax.rsqrt(mean_sq + 1e-05) * gain_ref[...])
    for m in range(mdl):
        piece = jnp.concatenate([v[m * sub : (m + 1) * sub] for v in normed], axis=0)
        send_x[m] = piece.astype(BF16)

    pl.semaphore_wait(barrier, n - 1)

    def remote(src, dst, ss, rs, to):
        return pltpu.make_async_remote_copy(
            src_ref=src, dst_ref=dst, send_sem=ss, recv_sem=rs,
            device_id={"hid": to}, device_id_type=MESH,
        )

    def landed(ref, sem):
        remote(ref, ref, x_s, sem, partner).wait_recv()

    def sent(ref, sem):
        remote(ref, ref, sem, ret_r.at[0], partner).wait_send()

    def loop(lo, hi, f):
        def body(i, carry):
            f(i)
            return carry

        lax.fori_loop(lo, hi, body, 0)

    def far_dev(k):
        ahead, way = k // mdl, k % mdl
        turn = (way // quad + 1 + group) % 2 * quad + (member + way) % quad
        return (group + 1 + ahead) % groups * mdl + (turn if FARTHEST else (member + way) % mdl)

    def near_dev(d):
        return base + (member + d) % mdl

    def x_copy(to, sem):
        return remote(send_x.at[to % mdl], arrived.at[me], x_s, sem, to)

    loop(0, far_n, lambda k: x_copy(far_dev(k), x_r.at[FAR]).start())
    loop(1, mdl, lambda d: x_copy(near_dev(d), x_r.at[NEAR]).start())
    arrived[me] = send_x[member]
    acc[...] = jnp.zeros_like(acc)

    def widen(at, src):
        wide[pl.ds(pl.multiple_of(at * tile, tile), tile), :] = arrived[src].astype(F32)

    if DOWN_AT == 1:
        start_weights(2, 0, blocks)
    landed(arrived.at[pl.ds(0, mdl - 1)], x_r.at[NEAR])
    loop(0, mdl, lambda m: widen(far_n + m, base + m))
    landed(arrived.at[pl.ds(0, far_n)], x_r.at[FAR])
    if DOWN_AT == 2:
        start_weights(2, 0, blocks)
    loop(0, far_n, lambda k: widen(k, (base + mdl + k) % n))
    for j in range(sub):
        x_vm[:, j * hd : (j + 1) * hd] = wide[pl.ds(j, batch, stride=sub), :].astype(BF16)
    weights_here(0, gate_vm)

    def pair_cols(vm, i, c):
        at = i * cb + c * 2
        return jnp.concatenate([vm[list_ref[group, at + b]] for b in range(2)], axis=1)

    def pack(y, s, i, c):
        for q in range(chips):
            for p in range(2):
                lo = part_at[p] + q * rp[p]
                y_q = y[lo : lo + rp[p]]
                pair_out[s, i, c, q, span[p], :] = jnp.concatenate(
                    [y_q[:, :bw], y_q[:, bw:]], axis=0
                ).astype(BF16)

    def gate_chunk(i):
        x = x_vm[...]
        for c in range(2):
            y = jnp.dot(x, pair_cols(gate_vm, i, c), preferred_element_type=F32)
            pack(y, 0, i, c)

    def up_chunk(i):
        x = x_vm[...]
        for c in range(2):
            y = jnp.dot(x, pair_cols(up_vm, i, c), preferred_element_type=F32)
            pack(y, 1, i, c)

    both = pl.ds(0, 2 * (rp[0] + rp[1]))

    def pair_copy(s, at, row, sem):
        return remote(
            pair_out.at[s, at, 1 - core, :, row], pair_in.at[s, at, :, row], pair_s, sem, partner
        )

    def add_pair(s, at, row):
        total = pair_out[s, at, core, :, row].astype(F32) + pair_in[s, at, :, row].astype(F32)
        chip_out[s, at, :, row] = total.astype(BF16)

    def chip_start(s, at, row, sem):
        for k in range(1, chips):
            to = (chip + k) % chips
            remote(
                chip_out.at[s, at, to, row], chip_in.at[s, at, k - 1, row], chip_s, sem,
                base + to * 2 + core,
            ).start()

    def total_of(s, i, row):
        total = chip_out[s, i, chip, row].astype(F32)
        for k in range(1, chips):
            total = total + chip_in[s, i, k - 1, row].astype(F32)
        return total

    def make_hidden(i, which):
        for p in which:
            gate, up = total_of(0, i, span[p]), total_of(1, i, span[p])
            row = lax.broadcasted_iota(jnp.int32, gate.shape, 0)
            active = row < (count_ref[group] - (i * cb + core * 2)) * rp[p]
            hid_all[i, core, chip, span[p], :] = jnp.where(
                active, jnp.maximum(gate, 0.0) * up, 0.0
            ).astype(BF16)

    def hid_start(at, row, sem):
        for k in range(1, chips):
            to = (chip + k) % chips
            ref = hid_all.at[at, core, chip, row]
            remote(ref, ref, hid_s, sem, base + to * 2 + core).start()

    def cross_start(at, row, sem):
        for k in range(chips):
            to = (chip + (k + 1) % chips) % chips
            ref = hid_all.at[at, core, chip, row]
            remote(ref, ref, fwd_s, sem, base + to * 2 + (1 - core)).start()

    def hid_landed(at, row, sem):
        landed(hid_all.at[at, 0, pl.ds(0, chips - 1), row], sem)

    def fwd_copy(at, row, sem):
        ref = hid_all.at[at, core, :, row]
        return remote(ref, ref, fwd_s, sem, partner)

    def down(i, which):
        at = pl.ds(part_at[which[0]], sum(part_rows[p] for p in which))
        total = acc[at, :]
        for c in range(2):
            parts = []
            for p in which:
                for q in range(chips):
                    two = hid_all[i, c, q, span[p], :].astype(F32)
                    parts.append(jnp.concatenate([two[: rp[p]], two[rp[p] :]], axis=1))
            lhs = jnp.concatenate(parts, axis=0).astype(BF16)
            w = jnp.concatenate(
                [down_vm[list_ref[group, i * cb + c * 2 + b]] for b in range(2)], axis=0
            )
            total = total + jnp.dot(lhs, w, preferred_element_type=F32)
        acc[at, :] = total

    gate_sets, near_sets = cut(nch, GATE_SETS), near_cut(nch)
    G0, N0 = 0, len(gate_sets)
    far_sets = cut(nch, FAR_SETS)
    C0 = N0 + len(near_sets)

    def ats(lo_hi):
        lo, hi = lo_hi
        return pl.ds(lo, hi - lo)

    def far_row(g):
        return both if far_sets[g][1] <= JOINT else span[FAR]

    def far_parts(g):
        return (FAR, NEAR) if far_sets[g][1] <= JOINT else (FAR,)

    def gate_set(g):
        for i in range(*gate_sets[g]):
            gate_chunk(i)
        pair_copy(0, ats(gate_sets[g]), both, pair_r.at[G0 + g]).start()

    def gate_add(g):
        landed(pair_in.at[0, ats(gate_sets[g]), :, both], pair_r.at[G0 + g])
        loop(*gate_sets[g], lambda i: add_pair(0, i, both))
        if GATE_WHOLE:
            chip_start(0, ats(gate_sets[g]), both, chip_r.at[G0 + g])
        else:
            chip_start(0, ats(gate_sets[g]), span[FAR], chip_r.at[G0 + g])
            chip_start(0, ats(gate_sets[g]), span[NEAR], chip_r.at[G0 + g])

    def gate_land(g):
        landed(chip_in.at[0, ats(gate_sets[g]), :, both], chip_r.at[G0 + g])

    def far_up(g):
        for i in range(*far_sets[g]):
            up_chunk(i)
        pair_copy(1, ats(far_sets[g]), far_row(g), pair_r.at[C0 + g]).start()

    def far_add(g):
        landed(pair_in.at[1, ats(far_sets[g]), :, far_row(g)], pair_r.at[C0 + g])
        for i in range(*far_sets[g]):
            add_pair(1, i, far_row(g))
        chip_start(1, ats(far_sets[g]), far_row(g), chip_r.at[C0 + g])

    def near_pair(g):
        pair_copy(1, ats(near_sets[g]), span[NEAR], pair_r.at[N0 + g]).start()

    def far_hidden(g):
        at = ats(far_sets[g])
        landed(chip_in.at[1, at, :, far_row(g)], chip_r.at[C0 + g])
        for i in range(*far_sets[g]):
            make_hidden(i, far_parts(g))
        hid_start(at, far_row(g), hid_r.at[C0 + g])
        if g in DIRECT:
            cross_start(at, far_row(g), fwd_r.at[C0 + g])

    def far_forward(g):
        hid_landed(ats(far_sets[g]), far_row(g), hid_r.at[C0 + g])
        if g not in DIRECT:
            fwd_copy(ats(far_sets[g]), far_row(g), fwd_r.at[C0 + g]).start()

    def far_down(g):
        landed(hid_all.at[ats(far_sets[g]), 0, :, far_row(g)], fwd_r.at[C0 + g])
        for i in range(*far_sets[g]):
            down(i, far_parts(g))

    def near_add(g):
        landed(pair_in.at[1, ats(near_sets[g]), :, span[NEAR]], pair_r.at[N0 + g])
        loop(*near_sets[g], lambda i: add_pair(1, i, span[NEAR]))
        chip_start(1, ats(near_sets[g]), span[NEAR], chip_r.at[N0 + g])

    def near_hidden(g):
        landed(chip_in.at[1, ats(near_sets[g]), :, span[NEAR]], chip_r.at[N0 + g])
        loop(*near_sets[g], lambda i: make_hidden(i, (NEAR,)))
        hid_start(ats(near_sets[g]), span[NEAR], hid_r.at[N0 + g])

    def near_forward(g):
        hid_landed(ats(near_sets[g]), span[NEAR], hid_r.at[N0 + g])
        fwd_copy(ats(near_sets[g]), span[NEAR], fwd_r.at[N0 + g]).start()

    def near_down(g):
        landed(hid_all.at[ats(near_sets[g]), 0, :, span[NEAR]], fwd_r.at[N0 + g])
        loop(*near_sets[g], lambda i: down(i, (NEAR,)))

    def down_here(_):
        weights_here(2, down_vm)

    def narrow(k):
        ret_out[k] = wide[pl.ds(pl.multiple_of(k * tile, tile), tile), :].astype(BF16)

    def spread(p):
        for j in range(sub):
            wide[pl.ds(part_at[p] * sub + j, part_rows[p], stride=sub), :] = acc[
                pl.ds(part_at[p], part_rows[p]), j * hd : (j + 1) * hd
            ]

    def far_slot(k):
        to = far_dev(k)
        return (to - base - mdl + n) % n

    def far_return(_):
        spread(FAR)

        def send(k):
            narrow(far_slot(k))
            remote(
                ret_out.at[far_slot(k)], ret_in.at[me], ret_s, ret_r.at[FAR], far_dev(k)
            ).start()

        loop(0, far_n, send)

    def near_return(_):
        spread(NEAR)
        loop(far_n, n, narrow)
        loop(
            1,
            mdl,
            lambda d: remote(
                ret_out.at[far_n + (member + d) % mdl], ret_in.at[me], ret_s,
                ret_r.at[NEAR], near_dev(d),
            ).start(),
        )
        ret_in[me] = ret_out[far_n + member]

    ops = []

    def put(f, count, first, step=1.0):
        for i in range(count):
            ops.append((first + i * step, len(ops), f, i))

    ng, nn, nf = len(gate_sets), len(near_sets), len(far_sets)
    put(gate_set, ng, -20)
    put(gate_add, ng, *T_GATE_ADD)
    put(lambda _: weights_here(1, up_vm), 1, -0.5)
    if DOWN_AT == 3:
        put(lambda _: start_weights(2, 0, blocks), 1, -3)
    for g, (lo, hi) in enumerate(far_sets):
        ops.append((hi - 1.0, len(ops), far_up, g))
    for g, (lo, hi) in enumerate(near_sets):
        ops.append((nch - 0.9, len(ops), near_pair, g))
    put(far_add, nf, *T_FAR_ADD)
    put(near_add, nn, *T_NEAR_ADD)
    put(gate_land, ng, T_FAR_HID[0] - 0.5, 0.01)
    put(far_hidden, nf, *T_FAR_HID)
    put(near_hidden, nn, *T_NEAR_HID)
    put(far_forward, nf, *T_FAR_FWD)
    put(down_here, 1, T_FAR_DOWN[0] - 0.05)
    put(far_down, nf, *T_FAR_DOWN)
    end = max(t for t, *_ in ops)
    put(far_return, 1, end + 1)
    put(near_forward, nn, *T_NEAR_FWD)
    put(near_down, nn, end + 20)
    put(near_return, 1, end + 30)
    for _, _, f, i in sorted(ops, key=lambda v: v[:2]):
        f(i)

    sent(arrived.at[pl.ds(0, n - 1)], x_s)
    sent(pair_in, pair_s)
    sent(chip_in, chip_s)
    sent(hid_all.at[:, 0, pl.ds(0, chips - 1)], hid_s)
    sent(hid_all.at[:, 0], fwd_s)
    landed(ret_in.at[pl.ds(0, mdl - 1)], ret_r.at[NEAR])
    landed(ret_in.at[pl.ds(0, far_n)], ret_r.at[FAR])
    for m in range(mdl):
        total = ret_in[m].astype(F32)
        for g in range(1, groups):
            total = total + ret_in[g * mdl + m].astype(F32)
        for r in range(rows):
            at = r * lanes + m * sub
            mixed[at : at + sub, :] = mixed[at : at + sub, :] + total[r * sub : (r + 1) * sub]
    for h in range(lanes):
        out_ref[:, h * hd : (h + 1) * hd] = mixed[pl.ds(h, rows, stride=lanes), :].astype(BF16)
    sent(ret_in.at[pl.ds(0, n - 1)], ret_s)


def on_device(
    queries, k_cache, v_cache, lengths, residual_in, norm_gain,
    gate_w, up_w, down_w, block_list, block_count,
):
    n = lax.axis_size("hid")
    rows, heads, hd = queries.shape
    cache = k_cache.shape[1]
    kv = k_cache.shape[2] // hd
    width = residual_in.shape[1]
    _, blocks, ds, bw = gate_w.shape
    mdl = width // ds
    cap = block_list.shape[1]
    cb = 4
    nch = cap // cb
    chips = mdl // 2
    batch = rows * n
    sub = ds // hd
    tile = rows * sub
    groups = n // mdl
    piece = 2 * batch // chips
    marks = len(cut(nch, GATE_SETS)) + len(near_cut(nch)) + len(cut(nch, FAR_SETS))
    dims = (n, mdl, rows, heads, hd, kv, cache, width, bw, cap, cb, blocks, groups)
    dma = pltpu.SemaphoreType.DMA
    vmem = pl.BlockSpec(memory_space=pltpu.VMEM)
    hbm = pl.BlockSpec(memory_space=pl.ANY)
    return pl.pallas_call(
        functools.partial(layer_kernel, dims),
        out_shape=pltpu.VMEM((rows, width), BF16),
        in_specs=[hbm] * 11,
        out_specs=vmem,
        scratch_shapes=[
            pltpu.VMEM(queries.shape, BF16),
            pltpu.VMEM(residual_in.shape, BF16),
            pltpu.VMEM((width // hd, hd), F32),
            pltpu.VMEM((rows, 2, cache, kv * hd), BF16),
            pltpu.VMEM(gate_w.shape[1:], BF16),
            pltpu.VMEM(up_w.shape[1:], BF16),
            pltpu.VMEM(down_w.shape[1:], BF16),
            pltpu.VMEM((rows * (width // hd), hd), F32),
            pltpu.VMEM((mdl, tile, hd), BF16),
            pltpu.VMEM((n, tile, hd), BF16),
            pltpu.VMEM((n * tile, hd), F32),
            pltpu.VMEM((batch, ds), BF16),
            pltpu.VMEM((2, nch, 2, chips, piece, bw), BF16),
            pltpu.VMEM((2, nch, chips, piece, bw), BF16),
            pltpu.VMEM((2, nch, chips, piece, bw), BF16),
            pltpu.VMEM((2, nch, chips - 1, piece, bw), BF16),
            pltpu.VMEM((nch, 2, chips, piece, bw), BF16),
            pltpu.VMEM((batch, ds), F32),
            pltpu.VMEM((n, tile, hd), BF16),
            pltpu.VMEM((n, tile, hd), BF16),
            dma((3,)),
            dma((rows,)),
            dma((3,)),
            dma(()),
            dma((2,)),
            dma(()),
            dma((marks,)),
            dma(()),
            dma((marks,)),
            dma(()),
            dma((marks,)),
            dma(()),
            dma((marks,)),
            dma(()),
            dma((2,)),
            pltpu.SMEM(lengths.shape, jnp.int32),
            pltpu.SMEM(block_list.shape, jnp.int32),
            pltpu.SMEM(block_count.shape, jnp.int32),
            dma((3,)),
        ],
        compiler_params=pltpu.CompilerParams(
            collective_id=0, has_side_effects=True, vmem_limit_bytes=63_000_000
        ),
        name="decode_layer",
    )(
        lengths, block_list, block_count, queries, residual_in,
        norm_gain.reshape(width // hd, hd), k_cache, v_cache, gate_w, up_w, down_w,
    )


def solution(mesh):
    in_specs = (
        P(("groups", "hid"), None, None),
        P(("groups", "hid"), None, None),
        P(("groups", "hid"), None, None),
        P(("groups", "hid")),
        P(("groups", "hid"), None),
        P(),
        P("hid", None, None, None),
        P("hid", None, None, None),
        P("hid", None, None, None),
        P("groups", None),
        P("groups"),
    )
    out_specs = P(("groups", "hid"), None)
    return jax.shard_map(
        on_device, mesh=mesh, in_specs=in_specs, out_specs=out_specs, check_vma=False
    )
```
